32 devices in a mesh: rep: 1 (over z), dp: 32 (over x, y, core).
Axes of the slice: x: 4, y: 4, z: 1, core: 2. Of those that a mesh axis runs over, the one named last changes fastest.
The devices are a block of a 4x4x8 slice.
Arguments:
- g_w_gate: bfloat16 [32, 2, 1024, 3200], P(('rep', 'dp'))
- g_w_up: bfloat16 [32, 2, 1024, 3200], P(('rep', 'dp'))
- g_w_down: bfloat16 [32, 2, 3200, 1024], P(('rep', 'dp'))
- w_gate: bfloat16 [2, 1024, 3200], replicated
- w_up: bfloat16 [2, 1024, 3200], replicated
- w_down: bfloat16 [2, 3200, 1024], replicated
- m_w_gate: float32 [2, 1024, 3200], P(None, 'dp')
- m_w_up: float32 [2, 1024, 3200], P(None, 'dp')
- m_w_down: float32 [2, 3200, 1024], P(None, 'dp')
- v_w_gate: float32 [2, 1024, 3200], P(None, 'dp')
- v_w_up: float32 [2, 1024, 3200], P(None, 'dp')
- v_w_down: float32 [2, 3200, 1024], P(None, 'dp')
Outputs:
- output 1: bfloat16 [2, 1024, 3200], P('rep')
- output 2: bfloat16 [2, 1024, 3200], P('rep')
- output 3: bfloat16 [2, 3200, 1024], P('rep')
- output 4: float32 [2, 1024, 3200], P('rep', 'dp')
- output 5: float32 [2, 1024, 3200], P('rep', 'dp')
- output 6: float32 [2, 3200, 1024], P('rep', 'dp')
- output 7: float32 [2, 1024, 3200], P('rep', 'dp')
- output 8: float32 [2, 1024, 3200], P('rep', 'dp')
- output 9: float32 [2, 3200, 1024], P('rep', 'dp')
All inputs are finite; a program needn't handle non-finite values.
Results may differ from the reference program's by a relative error of at most 0.022.
Values are sent between devices in bfloat16 or wider.
A program may use at most 768 MiB of HBM per device.

```python
import jax
import jax.numpy as jnp
from jax import lax

DEVICES = 32
D = 1024
FF = 3200
LAYERS = 2
NAMES = ("w_gate", "w_up", "w_down")
SHAPES = {"w_gate": (LAYERS, D, FF), "w_up": (LAYERS, D, FF), "w_down": (LAYERS, FF, D)}


def setup_inputs(seed: int = 0, part: int = 0) -> dict:
    kz, *keys = jax.random.split(jax.random.key(seed), 1 + 5 * len(NAMES))
    loud = 2.0 ** jax.random.uniform(kz, (), jnp.float32, -1.0, 1.0)
    drawn = {}
    for name, key, both in zip(NAMES, keys[:3], keys[3:6], strict=True):
        own = jax.random.normal(jax.random.fold_in(key, part), (DEVICES, *SHAPES[name]), jnp.float32)
        shared = jax.random.normal(jax.random.fold_in(both, part), SHAPES[name], jnp.float32)
        drawn["g_" + name] = (loud * (0.7 * shared / DEVICES + 0.7 * own * DEVICES**-0.5)).astype(jnp.bfloat16)
    for name, key in zip(NAMES, keys[6:9], strict=True):
        drawn[name] = (jax.random.normal(key, SHAPES[name], jnp.float32) * SHAPES[name][1] ** -0.5).astype(jnp.bfloat16)
    for name, key in zip(NAMES, keys[9:12], strict=True):
        drawn["m_" + name] = loud * 0.5 * jax.random.normal(key, SHAPES[name], jnp.float32)
    for name, key in zip(NAMES, keys[12:15], strict=True):
        drawn["v_" + name] = loud * loud * jax.random.uniform(key, SHAPES[name], jnp.float32, 0.5, 1.5)
    return drawn


def adamw(w, m, v, g):
    m = 0.9 * m + 0.1 * g
    v = 0.95 * v + 0.05 * g * g
    step = m * lax.rsqrt(v + 1e-8) + 0.1 * w
    return (w - 0.02 * step).astype(jnp.bfloat16), m, v


def clipped(gradients, sum_of_squares, count):
    factor = jnp.minimum(1.0, 0.5 * lax.rsqrt(sum_of_squares / count + 1e-30))
    return [g * factor for g in gradients]


def reference(g_w_gate, g_w_up, g_w_down, w_gate, w_up, w_down, m_w_gate, m_w_up, m_w_down, v_w_gate, v_w_up, v_w_down):
    def total(terms):
        return lax.scan(lambda so_far, term: (so_far + term.astype(jnp.float32), None), jnp.zeros(terms.shape[1:], jnp.float32), terms)[0]

    gradients = [total(terms).astype(jnp.bfloat16).astype(jnp.float32) for terms in (g_w_gate, g_w_up, g_w_down)]
    gradients = clipped(gradients, sum(jnp.sum(g * g) for g in gradients), sum(g.size for g in gradients))
    new = [
        adamw(w.astype(jnp.float32), m, v, g)
        for w, m, v, g in zip((w_gate, w_up, w_down), (m_w_gate, m_w_up, m_w_down), (v_w_gate, v_w_up, v_w_down), gradients, strict=True)
    ]
    return tuple(one[which] for which in range(3) for one in new)
```

```python
import functools
import math

import jax
import jax.numpy as jnp
from jax import lax
from jax.experimental import pallas as pl
from jax.experimental.pallas import tpu as pltpu
from jax.sharding import PartitionSpec as P

MESH = pl.DeviceIdType.MESH
CORES = 2
COLORS = 4
SLICES = 3
KEPT = COLORS // CORES
ANY = pl.BlockSpec(memory_space=pl.ANY)
VMEM = pl.BlockSpec(memory_space=pltpu.VMEM)
DMA = pltpu.SemaphoreType.DMA
ALL_VMEM = 67_043_328


def each(n, body):
    lax.fori_loop(0, n, lambda i, _: body(i), None)


class Place:
    def __init__(self, side):
        self.side = side
        self.me = lax.axis_index("dp")
        self.core = lax.rem(self.me, CORES)
        self.chip = self.me // CORES
        self.x, self.y = self.chip // side, lax.rem(self.chip, side)
        self.partner = self.me + 1 - 2 * self.core

    def at(self, x, y):
        return (x * self.side + y) * CORES + self.core

    def moved(self, p, by):
        return lax.rem(p + by + 2 * self.side, self.side)

    def way(self, q):
        on_x = q < COLORS // 2
        return jnp.where(on_x, self.x, self.y), jnp.where(on_x, self.y, self.x), 1 - 2 * lax.rem(q, 2)

    def next(self, q, first):
        up = 1 - 2 * lax.rem(q, 2)
        on_x = (q < COLORS // 2) == first
        return self.at(jnp.where(on_x, self.moved(self.x, up), self.x), jnp.where(on_x, self.y, self.moved(self.y, up)))


def remote(src, dst, send, recv, device):
    return pltpu.make_async_remote_copy(
        src_ref=src, dst_ref=dst, send_sem=send, recv_sem=recv, device_id={"dp": device}, device_id_type=MESH
    )


def part(ref, k, layer, q, t, columns):
    if k < SLICES - 1:
        return ref.at[layer, t, :, q] if q < COLORS // 2 else ref.at[layer, :, t, q]
    c = pl.ds(q * columns, columns)
    return ref.at[layer, t, :, :, c] if q < COLORS // 2 else ref.at[layer, :, t, :, c]


def wide(x):
    return x.astype(jnp.float32)


def squares(g):
    total = jnp.zeros((8, 128), jnp.float32)
    for r in range(0, g.shape[0], 8):
        for c in range(0, g.shape[1], 128):
            block = g[r : r + 8, c : c + 128]
            total += block * block
    return total


def scatter_kernel(side, n, *refs):
    terms, sums, total = refs[0:3], refs[3:6], refs[6]
    own, par, r1, r2 = refs[7:10], refs[10:13], refs[13:16], refs[16:19]
    fin, tmp, norms = refs[19:22], refs[22], refs[23]
    load, push_s, push_r, s1, v1, s2, v2, swap_s, swap_r, keep, norm_s, norm_r = refs[24:36]
    at = Place(side)
    me, core, partner = at.me, at.core, at.partner
    last = side - 1

    def group(q, s):
        p1, _, up = at.way(q)
        return at.moved(p1, -up * (1 + s))

    def loads(k, s):
        for q in range(COLORS):
            t = group(q, s)
            pltpu.make_async_copy(part(terms[k], k, core, q, t, own[k].shape[-1]), own[k].at[q, t], load.at[k, q, s]).start()

    def pushed(k, q, s, src=None):
        t = group(q, s)
        dst = par[k].at[q, t]
        return remote(dst if src is None else src, dst, push_s.at[k, q, s], push_r.at[k, q, s], partner)

    def pushes(k, s):
        for q in range(COLORS):
            pushed(k, q, s, part(terms[k], k, 1 - core, q, group(q, s), own[k].shape[-1])).start()

    def ready(k, q, s):
        t = group(q, s)
        pltpu.make_async_copy(own[k].at[q, t], own[k].at[q, t], load.at[k, q, s]).wait()
        pushed(k, q, s).wait_recv()

    def hop1(k, q, s):
        src = own[k].at[q, group(q, s)] if s == 0 else r1[k].at[q, s - 1]
        return remote(src, r1[k].at[q, s], s1.at[k, q, s], v1.at[k, q, s], at.next(q, True))

    def hop2(k, q, s):
        _, p2, up = at.way(q)
        src = r1[k].at[q, last - 1, at.moved(p2, -up)] if s == 0 else r2[k].at[q, s - 1]
        return remote(src, r2[k].at[q, s], s2.at[k, q, s], v2.at[k, q, s], at.next(q, False))

    barrier = pltpu.get_barrier_semaphore()
    each(n - 1, lambda i: pl.semaphore_signal(barrier, inc=1, device_id={"dp": lax.rem(me + 1 + i, n)}, device_id_type=MESH))
    for k in range(SLICES):
        loads(k, 0)
    pl.semaphore_wait(barrier, n - 1)
    for k in range(SLICES):
        pushes(k, 0)

    for s in range(last):
        for k in range(SLICES):

            def first(q):
                t = group(q, s)
                if s:
                    hop1(k, q, s - 1).wait_recv()
                ready(k, q, s)

                def add(j):
                    here = wide(own[k][q, t, j]) + wide(par[k][q, t, j])
                    if s:
                        r1[k][q, s - 1, j] = (wide(r1[k][q, s - 1, j]) + here).astype(jnp.bfloat16)
                    else:
                        own[k][q, t, j] = here.astype(jnp.bfloat16)

                each(side, add)
                hop1(k, q, s).start()

            each(COLORS, first)
            loads(k, s + 1)
            pushes(k, s + 1)

    def here(k, q, u):
        p1, _, _ = at.way(q)
        return wide(own[k][q, p1, u]) + wide(par[k][q, p1, u]) + wide(r1[k][q, last - 1, u])

    for s in range(last):
        for k in range(SLICES):

            def second(q):
                _, p2, up = at.way(q)
                u = at.moved(p2, -up * (1 + s))
                if s:
                    hop2(k, q, s - 1).wait_recv()
                    r2[k][q, s - 1] = (wide(r2[k][q, s - 1]) + here(k, q, u)).astype(jnp.bfloat16)
                else:
                    hop1(k, q, last - 1).wait_recv()
                    ready(k, q, last)
                    r1[k][q, last - 1, u] = here(k, q, u).astype(jnp.bfloat16)
                hop2(k, q, s).start()

            each(COLORS, second)

    norms[me] = jnp.zeros((8, 128), jnp.float32)
    for k in range(SLICES):

        def end(q):
            _, p2, _ = at.way(q)
            hop2(k, q, last - 1).wait_recv()
            g = (wide(r2[k][q, last - 1]) + here(k, q, p2)).astype(jnp.bfloat16)
            norms[me] += squares(wide(g))
            if k < SLICES - 1:
                fin[k][q] = g
            else:
                tmp[...] = wide(g)
                half = tmp.shape[0] // CORES
                for h in range(CORES):
                    fin[k][h, q] = tmp[h * half : (h + 1) * half].astype(jnp.bfloat16)

        each(COLORS, end)

    def share(k, of):
        return fin[k].at[pl.ds(of * KEPT, KEPT)] if k < SLICES - 1 else fin[k].at[of]

    def norm(i):
        return remote(norms.at[me], norms.at[me], norm_s.at[i], norm_r.at[i], lax.rem(me + 1 + i, n))

    each(n - 1, lambda i: norm(i).start())
    swaps = [remote(share(k, 1 - core), sums[k].at[core], swap_s.at[k], swap_r.at[k], partner) for k in range(SLICES)]
    keeps = [pltpu.make_async_copy(share(k, core), sums[k].at[core], keep.at[k]) for k in range(SLICES)]
    for copy in swaps + keeps:
        copy.start()
    each(n - 1, lambda i: norm(i).wait_recv())
    total[...] = jnp.zeros((8, 128), jnp.float32)

    def tally(i):
        total[...] += norms[i]

    each(n, tally)
    each(n - 1, lambda i: norm(i).wait_send())
    for copy in keeps:
        copy.wait()
    for k in range(SLICES):
        remote(share(k, 1 - core), sums[k].at[1 - core], swap_s.at[k], swap_r.at[k], partner).wait_recv()
        swaps[k].wait_send()

        def drain(q):
            for s in range(side):
                pushed(k, q, s).wait_send()
            for s in range(last):
                hop1(k, q, s).wait_send()
                hop2(k, q, s).wait_send()

        each(COLORS, drain)


def factor_of(total, count):
    return jnp.minimum(1.0, 0.5 * lax.rsqrt(jnp.sum(total) / count + 1e-30))


def moments(m, v, g):
    return 0.9 * m + 0.1 * g, 0.95 * v + 0.05 * g * g


def new_weight(w, m, v, g):
    m, v = moments(m, v, g)
    return (w - 0.02 * (m * lax.rsqrt(v + 1e-8) + 0.1 * w)).astype(jnp.bfloat16)


def lanes_of(layers, rows, q, columns, layer):
    per_row = COLORS * columns // 128 * layers
    return [pl.ds((q * columns // 128 + i) * layers + layer, rows, stride=per_row) for i in range(columns // 128)]


def gather_kernel(side, count, *refs):
    total, sums, weights, m, v = refs[0], refs[1:4], refs[4:7], refs[7:10], refs[10:13]
    out = refs[13:16]
    gb, wb, mb, vb = refs[16:19], refs[19:22], refs[22:25], refs[25:28]
    half_w, tmp, lent = refs[28], refs[29], refs[30:32]
    load, swap_s, swap_r, s1, v1, s2, v2, push_s, push_r = refs[32:41]
    at = Place(side)
    me, core, partner = at.me, at.core, at.partner
    other = 1 - core
    last = side - 1
    down = SLICES - 1

    barrier = pltpu.get_barrier_semaphore()
    near = [partner] + [at.next(q, True) for q in range(COLORS)]
    for device in near:
        pl.semaphore_signal(barrier, inc=1, device_id={"dp": device}, device_id_type=MESH)
    sources = [[sums[k], weights[k].at[:, me if k < down else at.chip], m[k], v[k]] for k in range(SLICES)]
    copies = [
        [pltpu.make_async_copy(src, dst[k], load.at[k, i]) for i, (src, dst) in enumerate(zip(sources[k], (gb, wb, mb, vb), strict=True))]
        for k in range(SLICES)
    ]
    for copy in sum(copies, []):
        copy.start()
    pl.semaphore_wait(barrier, len(near))
    factor = factor_of(total[...], count)

    def mine(k, layer, q):
        p1, p2, _ = at.way(q)
        return out[k].at[layer, q, p1, p2]

    def swap(k, i, q, layer):
        return remote(lent[k].at[i], mine(k, layer, q), swap_s.at[k, i], swap_r.at[k, i], partner)

    def hop1(k, q, s):
        p1, p2, up = at.way(q)
        ref = out[k].at[core, q, p1, at.moved(p2, -up * s)]
        return remote(ref, ref, s1.at[k, q, s], v1.at[k, q, s], at.next(q, False))

    def hop2(k, q, s):
        p1, _, up = at.way(q)
        ref = out[k].at[core, q, at.moved(p1, -up * s)]
        return remote(ref, ref, s2.at[k, q, s], v2.at[k, q, s], at.next(q, True))

    def push(k, q, s, layer):
        p1, _, up = at.way(q)
        ref = out[k].at[layer, q, at.moved(p1, -up * s)]
        return remote(ref, ref, push_s.at[k, q, s], push_r.at[k, q, s], partner)

    for k in range(down):
        for copy in copies[k]:
            copy.wait()
        for layer in (other, core):
            for i in range(KEPT):
                p1, p2, _ = at.way(core * KEPT + i)
                w = new_weight(wide(wb[k][layer, i]), mb[k][layer, i], vb[k][layer, i], wide(gb[k][layer, i]) * factor)
                if layer is other:
                    lent[k][i] = w
                    swap(k, i, core * KEPT + i, other).start()
                else:
                    out[k][layer, core * KEPT + i, p1, p2] = w

    for copy in copies[down]:
        copy.wait()
    rows, columns = half_w.shape[-2:]
    half_swap = remote(half_w.at[1], half_w.at[2], swap_s.at[down, 0], swap_r.at[down, 0], partner)
    for slot in (1, 0):
        for layer in range(CORES):

            @pl.when((layer == core) == (slot == 0))
            def _(layer=layer, slot=slot):
                for q in range(COLORS):
                    tmp[...] = wide(wb[down][layer, :, q * columns : (q + 1) * columns])
                    start = lax.select(core == 0, 0, 1)
                    w = jnp.where(start == 0, tmp[0:rows], tmp[rows : 2 * rows])
                    where = lanes_of(CORES, rows, q, columns, layer)
                    one = jnp.concatenate([mb[down][i, :] for i in where], axis=1)
                    two = jnp.concatenate([vb[down][i, :] for i in where], axis=1)
                    half_w[slot, q] = new_weight(w, one, two, wide(gb[down][layer, q]) * factor)

        if slot:
            half_swap.start()

    for k in range(down):
        for i in range(KEPT):
            swap(k, i, other * KEPT + i, core).wait_recv()

        each(COLORS, lambda q, k=k: hop1(k, q, 0).start())
    half_swap.wait_recv()
    top = 2 * core
    for q in range(COLORS):
        p1, p2, _ = at.way(q)
        tmp[0:rows] = wide(half_w[top, q])
        tmp[rows : 2 * rows] = wide(half_w[2 - top, q])
        out[down][core, q, p1, p2] = tmp[...].astype(jnp.bfloat16)
        hop1(down, q, 0).start()

    for s in range(1, last):
        for k in range(SLICES):

            def first(q):
                hop1(k, q, s - 1).wait_recv()
                hop1(k, q, s).start()

            each(COLORS, first)
    for s in range(side):
        for k in range(SLICES):

            def second(q):
                if s:
                    hop2(k, q, s - 1).wait_recv()
                else:
                    hop1(k, q, last - 1).wait_recv()
                if s < last:
                    hop2(k, q, s).start()
                push(k, q, s, core).start()

            each(COLORS, second)

    for k in range(SLICES):

        def drain(q):
            for s in range(side):
                push(k, q, s, other).wait_recv()
                push(k, q, s, core).wait_send()
            for s in range(last):
                hop1(k, q, s).wait_send()
                hop2(k, q, s).wait_send()

        each(COLORS, drain)
        if k < down:
            for i in range(KEPT):
                swap(k, i, core * KEPT + i, other).wait_send()
    half_swap.wait_send()


def finish_kernel(side, count, *refs):
    whole, total, sums, m, v = refs[0:3], refs[3], refs[4:7], refs[7:10], refs[10:13]
    new, new_m, new_v = refs[13:16], refs[16:19], refs[19:22]
    gb, mb, vb = refs[22:25], refs[25:28], refs[28:31]
    write, load, store = refs[31:34]
    down = SLICES - 1
    copies = [
        [pltpu.make_async_copy(src[k], dst[k], load.at[k, i]) for i, (src, dst) in enumerate(((sums, gb), (m, mb), (v, vb)))]
        for k in range(SLICES)
    ]
    for copy in sum(copies, []):
        copy.start()
    for k in range(SLICES):
        for layer in range(CORES):
            for q in range(COLORS):

                def put(t, k=k, layer=layer, q=q):
                    pltpu.make_async_copy(
                        whole[k].at[layer, q, t], part(new[k], k, layer, q, t, whole[k].shape[-1]), write.at[k, layer, q, t]
                    ).start()

                each(side, put)
    factor = factor_of(total[...], count)
    for k in range(SLICES):
        for copy in copies[k]:
            copy.wait()
        for layer in range(CORES):
            if k < down:
                for i in range(KEPT):
                    one, two = moments(mb[k][layer, i], vb[k][layer, i], wide(gb[k][layer, i]) * factor)
                    mb[k][layer, i] = one
                    vb[k][layer, i] = two
            else:
                rows, columns = gb[k].shape[-2:]
                for q in range(COLORS):
                    g = wide(gb[k][layer, q]) * factor
                    for i, where in enumerate(lanes_of(CORES, rows, q, columns, layer)):
                        one, two = moments(mb[k][where, :], vb[k][where, :], g[:, i * 128 : (i + 1) * 128])
                        mb[k][where, :] = one
                        vb[k][where, :] = two
        pltpu.make_async_copy(mb[k], new_m[k], store.at[k, 0]).start()
        pltpu.make_async_copy(vb[k], new_v[k], store.at[k, 1]).start()
    for k in range(SLICES):
        pltpu.make_async_copy(mb[k], new_m[k], store.at[k, 0]).wait()
        pltpu.make_async_copy(vb[k], new_v[k], store.at[k, 1]).wait()
        for layer in range(CORES):

            def wrote(i, k=k, layer=layer):
                q, t = i // side, lax.rem(i, side)
                pltpu.make_async_copy(whole[k].at[layer, q, t], whole[k].at[layer, q, t], write.at[k, layer, q, t]).wait()

            each(COLORS * side, wrote)


def solution(mesh):
    n = mesh.shape["dp"]
    side = math.isqrt(n // CORES)
    bf16, f32 = jnp.bfloat16, jnp.float32
    shape = jax.ShapeDtypeStruct

    def step(*arrays):
        terms, weights, m, v = (arrays[i : i + 3] for i in (0, 3, 6, 9))
        layers, depth, wide_columns = weights[0].shape
        _, deep, columns = weights[2].shape
        chips = side * side
        high, tall = depth // chips // COLORS, deep // chips
        pieces = [(high, wide_columns)] * 2 + [(tall, columns // COLORS)]
        half = (COLORS, tall // CORES, columns // COLORS)
        count = sum(w.size for w in weights)

        views = [t.reshape(layers, side, side, COLORS, high, wide_columns) for t in terms[:2]]
        views.append(terms[2].reshape(layers, side, side, tall, columns))
        kept = [shape((layers, KEPT, high, wide_columns), bf16)] * 2 + [shape((layers, *half), bf16)]
        *sums, total = pl.pallas_call(
            functools.partial(scatter_kernel, side, n),
            name="scatter",
            out_shape=(*kept, shape((8, 128), f32)),
            in_specs=[ANY] * 3,
            out_specs=(ANY,) * 3 + (VMEM,),
            scratch_shapes=[
                *(pltpu.VMEM((COLORS, side, side, *p), bf16) for p in pieces),
                *(pltpu.VMEM((COLORS, side, side, *p), bf16) for p in pieces),
                *(pltpu.VMEM((COLORS, side - 1, side, *p), bf16) for p in pieces),
                *(pltpu.VMEM((COLORS, side - 1, *p), bf16) for p in pieces),
                *(pltpu.VMEM((COLORS, *p), bf16) for p in pieces[:2]),
                pltpu.VMEM((CORES, *half), bf16),
                pltpu.VMEM(pieces[2], f32),
                pltpu.VMEM((n, 8, 128), f32),
                *(DMA((SLICES, COLORS, side)) for _ in range(3)),
                *(DMA((SLICES, COLORS, side - 1)) for _ in range(4)),
                *(DMA((SLICES,)) for _ in range(3)),
                *(DMA((n - 1,)) for _ in range(2)),
            ],
            compiler_params=pltpu.CompilerParams(collective_id=0, has_side_effects=True, vmem_limit_bytes=ALL_VMEM),
        )(*views)

        def by_lanes(a):
            layers, rows, columns = a.shape
            a = a.transpose(1, 0, 2).reshape(rows, layers, columns // 128, 128)
            return a.transpose(0, 2, 1, 3).reshape(-1, 128)

        def by_rows(a, like):
            layers, rows, columns = like.shape
            a = a.reshape(rows, columns // 128, layers, 128).transpose(0, 2, 1, 3)
            return a.reshape(rows, layers, columns).transpose(1, 0, 2)

        own = [w.reshape(layers, n, KEPT, high, wide_columns) for w in weights[:2]]
        own.append(weights[2].reshape(layers, chips, tall, columns))
        ms, vs = ([a.reshape(layers, KEPT, high, wide_columns) for a in b[:2]] + [by_lanes(b[2])] for b in (m, v))
        state = [pltpu.VMEM(a.shape, f32) for a in ms]
        gathered = pl.pallas_call(
            functools.partial(gather_kernel, side, count),
            name="gather",
            out_shape=tuple(pltpu.VMEM((layers, COLORS, side, side, *p), bf16) for p in pieces),
            in_specs=[VMEM] + [ANY] * 12,
            out_specs=(VMEM,) * 3,
            scratch_shapes=[
                *(pltpu.VMEM(k.shape, bf16) for k in kept),
                *(pltpu.VMEM((layers, KEPT, high, wide_columns), bf16) for _ in range(2)),
                pltpu.VMEM((layers, tall, columns), bf16),
                *state,
                *state,
                pltpu.VMEM((CORES + 1, *half), bf16),
                pltpu.VMEM(pieces[2], f32),
                *(pltpu.VMEM((KEPT, *p), bf16) for p in pieces[:2]),
                DMA((SLICES, 4)),
                *(DMA((SLICES, KEPT)) for _ in range(2)),
                *(DMA((SLICES, COLORS, side - 1)) for _ in range(4)),
                *(DMA((SLICES, COLORS, side)) for _ in range(2)),
            ],
            compiler_params=pltpu.CompilerParams(collective_id=1, has_side_effects=True, vmem_limit_bytes=20 << 20),
        )(total, *sums, *own, *ms, *vs)

        gathered = [pltpu.with_memory_space_constraint(a, pltpu.VMEM) for a in gathered]
        outs = pl.pallas_call(
            functools.partial(finish_kernel, side, count),
            name="finish",
            out_shape=tuple(shape(a.shape, a.dtype) for a in (*[shape(t.shape, bf16) for t in views], *ms, *vs)),
            in_specs=[VMEM] * 4 + [ANY] * 9,
            out_specs=(ANY,) * 9,
            scratch_shapes=[
                *(pltpu.VMEM(k.shape, bf16) for k in kept),
                *state,
                *state,
                DMA((SLICES, CORES, COLORS, side)),
                DMA((SLICES, 3)),
                DMA((SLICES, 2)),
            ],
            compiler_params=pltpu.CompilerParams(vmem_limit_bytes=20 << 20),
        )(*gathered, total, *sums, *ms, *vs)
        new = [a.reshape(w.shape) for a, w in zip(outs[:3], weights, strict=True)]
        rest = [
            (by_rows(a, like) if i == SLICES - 1 else a.reshape(like.shape))
            for block in (outs[3:6], outs[6:9])
            for i, (a, like) in enumerate(zip(block, m, strict=True))
        ]
        return (*new, *rest)

    all_of, cut = P(None, None, None), P(None, "dp", None)
    return jax.shard_map(
        step,
        mesh=mesh,
        in_specs=(P(("rep", "dp"), None, None, None),) * 3 + (all_of,) * 3 + (cut,) * 6,
        out_specs=(P("rep", None, None),) * 3 + (P("rep", "dp", None),) * 6,
        check_vma=False,
    )
```

```python
import functools
import math

import jax
import jax.numpy as jnp
from jax import lax
from jax.experimental import pallas as pl
from jax.experimental.pallas import tpu as pltpu
from jax.sharding import PartitionSpec as P

MESH = pl.DeviceIdType.MESH
CORES = 2
COLORS = 4
SLICES = 3
KEPT = COLORS // CORES
ANY = pl.BlockSpec(memory_space=pl.ANY)
VMEM = pl.BlockSpec(memory_space=pltpu.VMEM)
DMA = pltpu.SemaphoreType.DMA
ALL_VMEM = 67_043_328


def each(n, body):
    lax.fori_loop(0, n, lambda i, _: body(i), None)


class Place:
    def __init__(self, side):
        self.side = side
        self.me = lax.axis_index("dp")
        self.core = lax.rem(self.me, CORES)
        self.chip = self.me // CORES
        self.x, self.y = self.chip // side, lax.rem(self.chip, side)
        self.partner = self.me + 1 - 2 * self.core

    def at(self, x, y):
        return (x * self.side + y) * CORES + self.core

    def moved(self, p, by):
        return lax.rem(p + by + 2 * self.side, self.side)

    def way(self, q):
        on_x = q < COLORS // 2
        return jnp.where(on_x, self.x, self.y), jnp.where(on_x, self.y, self.x), 1 - 2 * lax.rem(q, 2)

    def next(self, q, first):
        up = 1 - 2 * lax.rem(q, 2)
        on_x = (q < COLORS // 2) == first
        return self.at(jnp.where(on_x, self.moved(self.x, up), self.x), jnp.where(on_x, self.y, self.moved(self.y, up)))


def remote(src, dst, send, recv, device):
    return pltpu.make_async_remote_copy(
        src_ref=src, dst_ref=dst, send_sem=send, recv_sem=recv, device_id={"dp": device}, device_id_type=MESH
    )


def meet(at):
    barrier = pltpu.get_barrier_semaphore()
    near = [at.partner] + [at.next(q, True) for q in range(COLORS)]
    for device in near:
        pl.semaphore_signal(barrier, inc=1, device_id={"dp": device}, device_id_type=MESH)
    return lambda: pl.semaphore_wait(barrier, len(near))


def part(ref, k, layer, q, t, columns):
    if k < SLICES - 1:
        return ref.at[layer, t, :, q] if q < COLORS // 2 else ref.at[layer, :, t, q]
    c = pl.ds(q * columns, columns)
    return ref.at[layer, t, :, :, c] if q < COLORS // 2 else ref.at[layer, :, t, :, c]


def wide(x):
    return x.astype(jnp.float32)


def squares(g):
    total = jnp.zeros((8, 128), jnp.float32)
    for r in range(0, g.shape[0], 8):
        for c in range(0, g.shape[1], 128):
            block = g[r : r + 8, c : c + 128]
            total += block * block
    return total


def scatter_kernel(side, n, *refs):
    terms, sums, total = refs[0:3], refs[3:6], refs[6]
    own, par, r1, r2 = refs[7:10], refs[10:13], refs[13:16], refs[16:19]
    fin, tmp, norms = refs[19:22], refs[22], refs[23]
    load, push_s, push_r, s1, v1, s2, v2, swap_s, swap_r, keep, norm_s, norm_r = refs[24:36]
    piece_s, piece_r, s1_piece, v1_piece = refs[36:40]
    at = Place(side)
    me, core, partner = at.me, at.core, at.partner
    last = side - 1

    def group(q, s):
        p1, _, up = at.way(q)
        return at.moved(p1, -up * (1 + s))

    def loads(k, s):
        for q in range(COLORS):
            t = group(q, s)
            pltpu.make_async_copy(part(terms[k], k, core, q, t, own[k].shape[-1]), own[k].at[q, t], load.at[k, q, s]).start()

    def pushed(k, q, s, src=None):
        t = group(q, s)
        dst = par[k].at[q, t]
        return remote(dst if src is None else src, dst, push_s.at[k, q, s], push_r.at[k, q, s], partner)

    def pushes(k, s):
        for q in range(COLORS):
            pushed(k, q, s, part(terms[k], k, 1 - core, q, group(q, s), own[k].shape[-1])).start()

    def loaded(k, q, s):
        t = group(q, s)
        pltpu.make_async_copy(own[k].at[q, t], own[k].at[q, t], load.at[k, q, s]).wait()

    def ready(k, q, s):
        loaded(k, q, s)
        pushed(k, q, s).wait_recv()

    def hop1(k, q, s):
        src = own[k].at[q, group(q, s)] if s == 0 else r1[k].at[q, s - 1]
        return remote(src, r1[k].at[q, s], s1.at[k, q, s], v1.at[k, q, s], at.next(q, True))

    def hop2(k, q, s):
        _, p2, up = at.way(q)
        src = r1[k].at[q, last - 1, at.moved(p2, -up)] if s == 0 else r2[k].at[q, s - 1]
        return remote(src, r2[k].at[q, s], s2.at[k, q, s], v2.at[k, q, s], at.next(q, False))

    def pushed_piece(q, j, src=None):
        dst = par[0].at[q, group(q, 0), j]
        return remote(dst if src is None else src, dst, piece_s.at[q, j], piece_r.at[q, j], partner)

    def hop1_piece(q, j):
        return remote(own[0].at[q, group(q, 0), j], r1[0].at[q, 0, j], s1_piece.at[q, j], v1_piece.at[q, j], at.next(q, True))

    greet = meet(at)
    for k in range(SLICES):
        loads(k, 0)
    greet()
    for j in range(side):
        for q in range(COLORS):
            pushed_piece(q, j, part(terms[0], 0, 1 - core, q, group(q, 0), own[0].shape[-1]).at[j]).start()
    for k in range(1, SLICES):
        pushes(k, 0)
    for j in range(side):

        def start(q):
            t = group(q, 0)
            if j == 0:
                loaded(0, q, 0)
            pushed_piece(q, j).wait_recv()
            own[0][q, t, j] = (wide(own[0][q, t, j]) + wide(par[0][q, t, j])).astype(jnp.bfloat16)
            hop1_piece(q, j).start()

        each(COLORS, start)
    loads(0, 1)
    pushes(0, 1)

    for s in range(last):
        for k in range(SLICES):
            if s == 0 and k == 0:
                continue

            def first(q):
                t = group(q, s)
                if s == 1 and k == 0:
                    each(side, lambda j: hop1_piece(q, j).wait_recv())
                elif s:
                    hop1(k, q, s - 1).wait_recv()
                ready(k, q, s)

                def add(j):
                    here = wide(own[k][q, t, j]) + wide(par[k][q, t, j])
                    if s:
                        r1[k][q, s - 1, j] = (wide(r1[k][q, s - 1, j]) + here).astype(jnp.bfloat16)
                    else:
                        own[k][q, t, j] = here.astype(jnp.bfloat16)

                each(side, add)
                hop1(k, q, s).start()

            each(COLORS, first)
            loads(k, s + 1)
            pushes(k, s + 1)

    def here(k, q, u):
        p1, _, _ = at.way(q)
        return wide(own[k][q, p1, u]) + wide(par[k][q, p1, u]) + wide(r1[k][q, last - 1, u])

    for s in range(last):
        for k in range(SLICES):

            def second(q):
                _, p2, up = at.way(q)
                u = at.moved(p2, -up * (1 + s))
                if s:
                    hop2(k, q, s - 1).wait_recv()
                    r2[k][q, s - 1] = (wide(r2[k][q, s - 1]) + here(k, q, u)).astype(jnp.bfloat16)
                else:
                    hop1(k, q, last - 1).wait_recv()
                    ready(k, q, last)
                    r1[k][q, last - 1, u] = here(k, q, u).astype(jnp.bfloat16)
                hop2(k, q, s).start()

            each(COLORS, second)

    norms[me] = jnp.zeros((8, 128), jnp.float32)
    for k in range(SLICES):

        def end(q):
            _, p2, _ = at.way(q)
            hop2(k, q, last - 1).wait_recv()
            g = (wide(r2[k][q, last - 1]) + here(k, q, p2)).astype(jnp.bfloat16)
            norms[me] += squares(wide(g))
            if k < SLICES - 1:
                fin[k][q] = g
            else:
                tmp[...] = wide(g)
                half = tmp.shape[0] // CORES
                for h in range(CORES):
                    fin[k][h, q] = tmp[h * half : (h + 1) * half].astype(jnp.bfloat16)

        each(COLORS, end)

    def share(k, of):
        return fin[k].at[pl.ds(of * KEPT, KEPT)] if k < SLICES - 1 else fin[k].at[of]

    def norm(i):
        return remote(norms.at[me], norms.at[me], norm_s.at[i], norm_r.at[i], lax.rem(me + 1 + i, n))

    each(n - 1, lambda i: norm(i).start())
    swaps = [remote(share(k, 1 - core), sums[k].at[core], swap_s.at[k], swap_r.at[k], partner) for k in range(SLICES)]
    keeps = [pltpu.make_async_copy(share(k, core), sums[k].at[core], keep.at[k]) for k in range(SLICES)]
    for copy in swaps + keeps:
        copy.start()
    each(n - 1, lambda i: norm(i).wait_recv())
    total[...] = jnp.zeros((8, 128), jnp.float32)

    def tally(i):
        total[...] += norms[i]

    each(n, tally)
    each(n - 1, lambda i: norm(i).wait_send())
    for copy in keeps:
        copy.wait()
    for k in range(SLICES):
        remote(share(k, 1 - core), sums[k].at[1 - core], swap_s.at[k], swap_r.at[k], partner).wait_recv()
        swaps[k].wait_send()

        def drain(q):
            whole_from = 1 if k == 0 else 0
            for s in range(whole_from, side):
                pushed(k, q, s).wait_send()
            for s in range(last):
                if s >= whole_from:
                    hop1(k, q, s).wait_send()
                hop2(k, q, s).wait_send()
            if whole_from:

                def pieces(j):
                    pushed_piece(q, j).wait_send()
                    hop1_piece(q, j).wait_send()

                each(side, pieces)

        each(COLORS, drain)


def factor_of(total, count):
    return jnp.minimum(1.0, 0.5 * lax.rsqrt(jnp.sum(total) / count + 1e-30))


def moments(m, v, g):
    return 0.9 * m + 0.1 * g, 0.95 * v + 0.05 * g * g


def new_weight(w, m, v, g):
    m, v = moments(m, v, g)
    return (w - 0.02 * (m * lax.rsqrt(v + 1e-8) + 0.1 * w)).astype(jnp.bfloat16)


def lanes_of(layers, rows, q, columns, layer):
    per_row = COLORS * columns // 128 * layers
    return [pl.ds((q * columns // 128 + i) * layers + layer, rows, stride=per_row) for i in range(columns // 128)]


def gather_kernel(side, count, *refs):
    total, sums, weights, m, v = refs[0], refs[1:4], refs[4:7], refs[7:10], refs[10:13]
    out, mb, vb = refs[13:16], refs[16:19], refs[19:22]
    gb, wb = refs[22:25], refs[25:28]
    half_w, tmp, lent = refs[28], refs[29], refs[30:32]
    load, swap_s, swap_r, s1, v1, s2, v2, push_s, push_r = refs[32:41]
    s2_piece, v2_piece, piece_s, piece_r = refs[41:45]
    at = Place(side)
    me, core, partner = at.me, at.core, at.partner
    other = 1 - core
    last = side - 1
    down = SLICES - 1

    greet = meet(at)
    sources = [[sums[k], weights[k].at[:, me if k < down else at.chip], m[k], v[k]] for k in range(SLICES)]
    copies = [
        [pltpu.make_async_copy(src, dst[k], load.at[k, i]) for i, (src, dst) in enumerate(zip(sources[k], (gb, wb, mb, vb), strict=True))]
        for k in range(SLICES)
    ]
    for copy in sum(copies, []):
        copy.start()
    greet()
    factor = factor_of(total[...], count)

    def mine(k, layer, q):
        p1, p2, _ = at.way(q)
        return out[k].at[layer, q, p1, p2]

    def swap(k, i, q, layer):
        return remote(lent[k].at[i], mine(k, layer, q), swap_s.at[k, i], swap_r.at[k, i], partner)

    def hop1(k, q, s):
        p1, p2, up = at.way(q)
        ref = out[k].at[core, q, p1, at.moved(p2, -up * s)]
        return remote(ref, ref, s1.at[k, q, s], v1.at[k, q, s], at.next(q, False))

    def hop2(k, q, s):
        p1, _, up = at.way(q)
        ref = out[k].at[core, q, at.moved(p1, -up * s)]
        return remote(ref, ref, s2.at[k, q, s], v2.at[k, q, s], at.next(q, True))

    def push(k, q, s, layer):
        p1, _, up = at.way(q)
        ref = out[k].at[layer, q, at.moved(p1, -up * s)]
        return remote(ref, ref, push_s.at[k, q, s], push_r.at[k, q, s], partner)

    def hop2_piece(q, j):
        p1, _, up = at.way(q)
        ref = out[down].at[core, q, at.moved(p1, -up * (last - 1)), j]
        return remote(ref, ref, s2_piece.at[q, j], v2_piece.at[q, j], at.next(q, True))

    def push_piece(q, j, layer):
        p1, _, up = at.way(q)
        ref = out[down].at[layer, q, at.moved(p1, -up * last), j]
        return remote(ref, ref, piece_s.at[q, j], piece_r.at[q, j], partner)

    def step(k):
        for copy in copies[k]:
            copy.wait()
        for layer in (other, core):
            for i in range(KEPT):
                q = core * KEPT + i
                w = new_weight(wide(wb[k][layer, i]), mb[k][layer, i], vb[k][layer, i], wide(gb[k][layer, i]) * factor)
                if layer is other:
                    lent[k][i] = w
                    swap(k, i, q, other).start()
                else:
                    p1, p2, _ = at.way(q)
                    out[k][layer, q, p1, p2] = w
                    hop1(k, q, 0).start()

    def swapped(k):
        for i in range(KEPT):
            q = other * KEPT + i
            swap(k, i, q, core).wait_recv()
            hop1(k, q, 0).start()

    rows, columns = half_w.shape[-2:]
    half_swap = remote(half_w.at[1], half_w.at[2], swap_s.at[down, 0], swap_r.at[down, 0], partner)

    def step_down(slot):
        for layer in range(CORES):

            @pl.when((layer == core) == (slot == 0))
            def _(layer=layer):
                for q in range(COLORS):
                    tmp[...] = wide(wb[down][layer, :, q * columns : (q + 1) * columns])
                    w = jnp.where(core == 0, tmp[0:rows], tmp[rows : 2 * rows])
                    where = lanes_of(CORES, rows, q, columns, layer)
                    one = jnp.concatenate([mb[down][i, :] for i in where], axis=1)
                    two = jnp.concatenate([vb[down][i, :] for i in where], axis=1)
                    half_w[slot, q] = new_weight(w, one, two, wide(gb[down][layer, q]) * factor)

    def keep_moments(k):
        for layer in range(CORES):
            if k < down:
                for i in range(KEPT):
                    one, two = moments(mb[k][layer, i], vb[k][layer, i], wide(gb[k][layer, i]) * factor)
                    mb[k][layer, i] = one
                    vb[k][layer, i] = two
            else:
                for q in range(COLORS):
                    g = wide(gb[k][layer, q]) * factor
                    for i, where in enumerate(lanes_of(CORES, rows, q, columns, layer)):
                        one, two = moments(mb[k][where, :], vb[k][where, :], g[:, i * 128 : (i + 1) * 128])
                        mb[k][where, :] = one
                        vb[k][where, :] = two

    step(0)
    step(1)
    swapped(0)
    for copy in copies[down]:
        copy.wait()
    step_down(1)
    half_swap.start()
    swapped(1)
    step_down(0)
    half_swap.wait_recv()
    top = 2 * core
    for q in range(COLORS):
        p1, p2, _ = at.way(q)
        tmp[0:rows] = wide(half_w[top, q])
        tmp[rows : 2 * rows] = wide(half_w[2 - top, q])
        out[down][core, q, p1, p2] = tmp[...].astype(jnp.bfloat16)
        hop1(down, q, 0).start()

    for s in range(1, last):
        for k in range(SLICES):

            def first(q):
                hop1(k, q, s - 1).wait_recv()
                hop1(k, q, s).start()

            each(COLORS, first)
    for s in range(side):
        for k in range(SLICES):

            def second(q):
                if s:
                    hop2(k, q, s - 1).wait_recv()
                else:
                    hop1(k, q, last - 1).wait_recv()
                if k == down and s == last - 1:
                    each(side, lambda j: hop2_piece(q, j).start())
                elif s < last:
                    hop2(k, q, s).start()
                push(k, q, s, core).start()

            if k == down and s == last:

                def end(i):
                    j, q = i // COLORS, lax.rem(i, COLORS)
                    hop2_piece(q, j).wait_recv()
                    push_piece(q, j, core).start()

                each(side * COLORS, end)
            else:
                each(COLORS, second)
            if s == 0:
                keep_moments(k)

    for k in range(SLICES):

        def drain(q):
            cut = 1 if k == down else 0
            for s in range(side - cut):
                push(k, q, s, other).wait_recv()
                push(k, q, s, core).wait_send()
            for s in range(last):
                hop1(k, q, s).wait_send()
                if s < last - cut:
                    hop2(k, q, s).wait_send()
            if cut:

                def pieces(j):
                    push_piece(q, j, other).wait_recv()
                    push_piece(q, j, core).wait_send()
                    hop2_piece(q, j).wait_send()

                each(side, pieces)

        each(COLORS, drain)
        if k < down:
            for i in range(KEPT):
                swap(k, i, core * KEPT + i, other).wait_send()
    half_swap.wait_send()


def finish_kernel(side, *refs):
    whole, state, new, new_state, write, store = refs[0:3], refs[3:9], refs[9:12], refs[12:18], refs[18], refs[19]
    for k in range(SLICES):
        for layer in range(CORES):
            for q in range(COLORS):

                def put(t, k=k, layer=layer, q=q):
                    src, dst = whole[k].at[layer, q, t], part(new[k], k, layer, q, t, whole[k].shape[-1])
                    pltpu.make_async_copy(src, dst, write.at[k, layer, q, t]).start()

                each(side, put)
    copies = [pltpu.make_async_copy(src, dst, store.at[i]) for i, (src, dst) in enumerate(zip(state, new_state, strict=True))]
    for copy in copies:
        copy.start()
    for copy in copies:
        copy.wait()
    for k in range(SLICES):
        for layer in range(CORES):

            def wrote(i, k=k, layer=layer):
                q, t = i // side, lax.rem(i, side)
                pltpu.make_async_copy(whole[k].at[layer, q, t], whole[k].at[layer, q, t], write.at[k, layer, q, t]).wait()

            each(COLORS * side, wrote)


def solution(mesh):
    n = mesh.shape["dp"]
    side = math.isqrt(n // CORES)
    bf16, f32 = jnp.bfloat16, jnp.float32
    shape = jax.ShapeDtypeStruct

    def step(*arrays):
        terms, weights, m, v = (arrays[i : i + 3] for i in (0, 3, 6, 9))
        layers, depth, wide_columns = weights[0].shape
        _, deep, columns = weights[2].shape
        chips = side * side
        high, tall = depth // chips // COLORS, deep // chips
        pieces = [(high, wide_columns)] * 2 + [(tall, columns // COLORS)]
        half = (COLORS, tall // CORES, columns // COLORS)
        count = sum(w.size for w in weights)

        views = [t.reshape(layers, side, side, COLORS, high, wide_columns) for t in terms[:2]]
        views.append(terms[2].reshape(layers, side, side, tall, columns))
        kept = [shape((layers, KEPT, high, wide_columns), bf16)] * 2 + [shape((layers, *half), bf16)]
        *sums, total = pl.pallas_call(
            functools.partial(scatter_kernel, side, n),
            name="scatter",
            out_shape=(*kept, shape((8, 128), f32)),
            in_specs=[ANY] * 3,
            out_specs=(ANY,) * 3 + (VMEM,),
            scratch_shapes=[
                *(pltpu.VMEM((COLORS, side, side, *p), bf16) for p in pieces),
                *(pltpu.VMEM((COLORS, side, side, *p), bf16) for p in pieces),
                *(pltpu.VMEM((COLORS, side - 1, side, *p), bf16) for p in pieces),
                *(pltpu.VMEM((COLORS, side - 1, *p), bf16) for p in pieces),
                *(pltpu.VMEM((COLORS, *p), bf16) for p in pieces[:2]),
                pltpu.VMEM((CORES, *half), bf16),
                pltpu.VMEM(pieces[2], f32),
                pltpu.VMEM((n, 8, 128), f32),
                *(DMA((SLICES, COLORS, side)) for _ in range(3)),
                *(DMA((SLICES, COLORS, side - 1)) for _ in range(4)),
                *(DMA((SLICES,)) for _ in range(3)),
                *(DMA((n - 1,)) for _ in range(2)),
                *(DMA((COLORS, side)) for _ in range(4)),
            ],
            compiler_params=pltpu.CompilerParams(collective_id=0, has_side_effects=True, vmem_limit_bytes=ALL_VMEM),
        )(*views)

        def by_lanes(a):
            layers, rows, columns = a.shape
            a = a.transpose(1, 0, 2).reshape(rows, layers, columns // 128, 128)
            return a.transpose(0, 2, 1, 3).reshape(-1, 128)

        def by_rows(a, like):
            layers, rows, columns = like.shape
            a = a.reshape(rows, columns // 128, layers, 128).transpose(0, 2, 1, 3)
            return a.reshape(rows, layers, columns).transpose(1, 0, 2)

        own = [w.reshape(layers, n, KEPT, high, wide_columns) for w in weights[:2]]
        own.append(weights[2].reshape(layers, chips, tall, columns))
        ms, vs = ([a.reshape(layers, KEPT, high, wide_columns) for a in b[:2]] + [by_lanes(b[2])] for b in (m, v))
        state = [pltpu.VMEM(a.shape, f32) for a in ms]
        gathered = pl.pallas_call(
            functools.partial(gather_kernel, side, count),
            name="gather",
            out_shape=(*(pltpu.VMEM((layers, COLORS, side, side, *p), bf16) for p in pieces), *state, *state),
            in_specs=[VMEM] + [ANY] * 12,
            out_specs=(VMEM,) * 9,
            scratch_shapes=[
                *(pltpu.VMEM(k.shape, bf16) for k in kept),
                *(pltpu.VMEM((layers, KEPT, high, wide_columns), bf16) for _ in range(2)),
                pltpu.VMEM((layers, tall, columns), bf16),
                pltpu.VMEM((CORES + 1, *half), bf16),
                pltpu.VMEM(pieces[2], f32),
                *(pltpu.VMEM((KEPT, *p), bf16) for p in pieces[:2]),
                DMA((SLICES, 4)),
                *(DMA((SLICES, KEPT)) for _ in range(2)),
                *(DMA((SLICES, COLORS, side - 1)) for _ in range(4)),
                *(DMA((SLICES, COLORS, side)) for _ in range(2)),
                *(DMA((COLORS, side)) for _ in range(4)),
            ],
            compiler_params=pltpu.CompilerParams(collective_id=1, has_side_effects=True, vmem_limit_bytes=8 << 20),
        )(total, *sums, *own, *ms, *vs)

        gathered = [pltpu.with_memory_space_constraint(a, pltpu.VMEM) for a in gathered]
        outs = pl.pallas_call(
            functools.partial(finish_kernel, side),
            name="finish",
            out_shape=tuple(shape(a.shape, a.dtype) for a in (*[shape(t.shape, bf16) for t in views], *ms, *vs)),
            in_specs=[VMEM] * 9,
            out_specs=(ANY,) * 9,
            scratch_shapes=[DMA((SLICES, CORES, COLORS, side)), DMA((2 * SLICES,))],
            compiler_params=pltpu.CompilerParams(vmem_limit_bytes=1 << 20),
        )(*gathered)
        new = [a.reshape(w.shape) for a, w in zip(outs[:3], weights, strict=True)]
        rest = [
            (by_rows(a, like) if i == SLICES - 1 else a.reshape(like.shape))
            for block in (outs[3:6], outs[6:9])
            for i, (a, like) in enumerate(zip(block, m, strict=True))
        ]
        return (*new, *rest)

    all_of, cut = P(None, None, None), P(None, "dp", None)
    return jax.shard_map(
        step,
        mesh=mesh,
        in_specs=(P(("rep", "dp"), None, None, None),) * 3 + (all_of,) * 3 + (cut,) * 6,
        out_specs=(P("rep", None, None),) * 3 + (P("rep", "dp", None),) * 6,
        check_vma=False,
    )
```

```python
import functools
import math

import jax
import jax.numpy as jnp
from jax import lax
from jax.experimental import pallas as pl
from jax.experimental.pallas import tpu as pltpu
from jax.sharding import PartitionSpec as P

MESH = pl.DeviceIdType.MESH
CORES = 2
COLORS = 4
SLICES = 3
KEPT = COLORS // CORES
ANY = pl.BlockSpec(memory_space=pl.ANY)
VMEM = pl.BlockSpec(memory_space=pltpu.VMEM)
DMA = pltpu.SemaphoreType.DMA
ALL_VMEM = 67_043_328


def each(n, body):
    lax.fori_loop(0, n, lambda i, _: body(i), None)


class Place:
    def __init__(self, side):
        self.side = side
        self.me = lax.axis_index("dp")
        self.core = lax.rem(self.me, CORES)
        self.chip = self.me // CORES
        self.x, self.y = self.chip // side, lax.rem(self.chip, side)
        self.partner = self.me + 1 - 2 * self.core

    def at(self, x, y):
        return (x * self.side + y) * CORES + self.core

    def moved(self, p, by):
        return lax.rem(p + by + 2 * self.side, self.side)

    def way(self, q):
        on_x = q < COLORS // 2
        return jnp.where(on_x, self.x, self.y), jnp.where(on_x, self.y, self.x), 1 - 2 * lax.rem(q, 2)

    def next(self, q, first):
        up = 1 - 2 * lax.rem(q, 2)
        on_x = (q < COLORS // 2) == first
        return self.at(jnp.where(on_x, self.moved(self.x, up), self.x), jnp.where(on_x, self.y, self.moved(self.y, up)))


def remote(src, dst, send, recv, device):
    return pltpu.make_async_remote_copy(
        src_ref=src, dst_ref=dst, send_sem=send, recv_sem=recv, device_id={"dp": device}, device_id_type=MESH
    )


def meet(at):
    barrier = pltpu.get_barrier_semaphore()
    near = [at.partner] + [at.next(q, True) for q in range(COLORS)]
    for device in near:
        pl.semaphore_signal(barrier, inc=1, device_id={"dp": device}, device_id_type=MESH)
    return lambda: pl.semaphore_wait(barrier, len(near))


def part(ref, k, layer, q, t, columns):
    if k < SLICES - 1:
        return ref.at[layer, t, :, q] if q < COLORS // 2 else ref.at[layer, :, t, q]
    c = pl.ds(q * columns, columns)
    return ref.at[layer, t, :, :, c] if q < COLORS // 2 else ref.at[layer, :, t, :, c]


def wide(x):
    return x.astype(jnp.float32)


def squares(g):
    total = jnp.zeros((8, 128), jnp.float32)
    for r in range(0, g.shape[0], 8):
        for c in range(0, g.shape[1], 128):
            block = g[r : r + 8, c : c + 128]
            total += block * block
    return total


def scatter_kernel(side, n, *refs):
    terms, sums, total = refs[0:3], refs[3:6], refs[6]
    own, par, r1, r2 = refs[7:10], refs[10:13], refs[13:16], refs[16:19]
    fin, tmp, norms = refs[19:22], refs[22], refs[23]
    load, push_s, push_r, s1, v1, s2, v2, swap_s, swap_r, keep, norm_s, norm_r = refs[24:36]
    piece_s, piece_r, s1_piece, v1_piece = refs[36:40]
    at = Place(side)
    me, core, partner = at.me, at.core, at.partner
    last = side - 1

    def group(q, s):
        p1, _, up = at.way(q)
        return at.moved(p1, -up * (1 + s))

    def loads(k, s):
        for q in range(COLORS):
            t = group(q, s)
            pltpu.make_async_copy(part(terms[k], k, core, q, t, own[k].shape[-1]), own[k].at[q, t], load.at[k, q, s]).start()

    def pushed(k, q, s, src=None):
        t = group(q, s)
        dst = par[k].at[q, t]
        return remote(dst if src is None else src, dst, push_s.at[k, q, s], push_r.at[k, q, s], partner)

    def pushes(k, s):
        for q in range(COLORS):
            pushed(k, q, s, part(terms[k], k, 1 - core, q, group(q, s), own[k].shape[-1])).start()

    def loaded(k, q, s):
        t = group(q, s)
        pltpu.make_async_copy(own[k].at[q, t], own[k].at[q, t], load.at[k, q, s]).wait()

    def ready(k, q, s):
        loaded(k, q, s)
        pushed(k, q, s).wait_recv()

    def hop1(k, q, s):
        src = own[k].at[q, group(q, s)] if s == 0 else r1[k].at[q, s - 1]
        return remote(src, r1[k].at[q, s], s1.at[k, q, s], v1.at[k, q, s], at.next(q, True))

    def hop2(k, q, s):
        _, p2, up = at.way(q)
        src = r1[k].at[q, last - 1, at.moved(p2, -up)] if s == 0 else r2[k].at[q, s - 1]
        return remote(src, r2[k].at[q, s], s2.at[k, q, s], v2.at[k, q, s], at.next(q, False))

    def pushed_piece(q, j, src=None):
        dst = par[0].at[q, group(q, 0), j]
        return remote(dst if src is None else src, dst, piece_s.at[q, j], piece_r.at[q, j], partner)

    def hop1_piece(q, j):
        return remote(own[0].at[q, group(q, 0), j], r1[0].at[q, 0, j], s1_piece.at[q, j], v1_piece.at[q, j], at.next(q, True))

    greet = meet(at)
    for k in range(SLICES):
        loads(k, 0)
    greet()
    for j in range(side):
        for q in range(COLORS):
            pushed_piece(q, j, part(terms[0], 0, 1 - core, q, group(q, 0), own[0].shape[-1]).at[j]).start()
    for k in range(1, SLICES):
        pushes(k, 0)
    for j in range(side):

        def start(q):
            t = group(q, 0)
            if j == 0:
                loaded(0, q, 0)
            pushed_piece(q, j).wait_recv()
            own[0][q, t, j] = (wide(own[0][q, t, j]) + wide(par[0][q, t, j])).astype(jnp.bfloat16)
            hop1_piece(q, j).start()

        each(COLORS, start)
    loads(0, 1)
    pushes(0, 1)

    for s in range(last):
        for k in range(SLICES):
            if s == 0 and k == 0:
                continue

            def first(q):
                t = group(q, s)
                if s == 1 and k == 0:
                    each(side, lambda j: hop1_piece(q, j).wait_recv())
                elif s:
                    hop1(k, q, s - 1).wait_recv()
                ready(k, q, s)

                def add(j):
                    here = wide(own[k][q, t, j]) + wide(par[k][q, t, j])
                    if s:
                        r1[k][q, s - 1, j] = (wide(r1[k][q, s - 1, j]) + here).astype(jnp.bfloat16)
                    else:
                        own[k][q, t, j] = here.astype(jnp.bfloat16)

                each(side, add)
                hop1(k, q, s).start()

            each(COLORS, first)
            loads(k, s + 1)
            pushes(k, s + 1)

    def here(k, q, u):
        p1, _, _ = at.way(q)
        return wide(own[k][q, p1, u]) + wide(par[k][q, p1, u]) + wide(r1[k][q, last - 1, u])

    for s in range(last):
        for k in range(SLICES):

            def second(q):
                _, p2, up = at.way(q)
                u = at.moved(p2, -up * (1 + s))
                if s:
                    hop2(k, q, s - 1).wait_recv()
                    r2[k][q, s - 1] = (wide(r2[k][q, s - 1]) + here(k, q, u)).astype(jnp.bfloat16)
                else:
                    hop1(k, q, last - 1).wait_recv()
                    ready(k, q, last)
                    r1[k][q, last - 1, u] = here(k, q, u).astype(jnp.bfloat16)
                hop2(k, q, s).start()

            each(COLORS, second)

    norms[me] = jnp.zeros((8, 128), jnp.float32)
    for k in range(SLICES):

        def end(q):
            _, p2, _ = at.way(q)
            hop2(k, q, last - 1).wait_recv()
            g = (wide(r2[k][q, last - 1]) + here(k, q, p2)).astype(jnp.bfloat16)
            norms[me] += squares(wide(g))
            if k < SLICES - 1:
                fin[k][q] = g
            else:
                tmp[...] = wide(g)
                half = tmp.shape[0] // CORES
                for h in range(CORES):
                    fin[k][h, q] = tmp[h * half : (h + 1) * half].astype(jnp.bfloat16)

        each(COLORS, end)

    def share(k, of):
        return fin[k].at[pl.ds(of * KEPT, KEPT)] if k < SLICES - 1 else fin[k].at[of]

    def norm(i):
        return remote(norms.at[me], norms.at[me], norm_s.at[i], norm_r.at[i], lax.rem(me + 1 + i, n))

    each(n - 1, lambda i: norm(i).start())
    swaps = [remote(share(k, 1 - core), sums[k].at[core], swap_s.at[k], swap_r.at[k], partner) for k in range(SLICES)]
    keeps = [pltpu.make_async_copy(share(k, core), sums[k].at[core], keep.at[k]) for k in range(SLICES)]
    for copy in swaps + keeps:
        copy.start()
    each(n - 1, lambda i: norm(i).wait_recv())
    total[...] = jnp.zeros((8, 128), jnp.float32)

    def tally(i):
        total[...] += norms[i]

    each(n, tally)
    each(n - 1, lambda i: norm(i).wait_send())
    for copy in keeps:
        copy.wait()
    for k in range(SLICES):
        remote(share(k, 1 - core), sums[k].at[1 - core], swap_s.at[k], swap_r.at[k], partner).wait_recv()
        swaps[k].wait_send()

        def drain(q):
            whole_from = 1 if k == 0 else 0
            for s in range(whole_from, side):
                pushed(k, q, s).wait_send()
            for s in range(last):
                if s >= whole_from:
                    hop1(k, q, s).wait_send()
                hop2(k, q, s).wait_send()
            if whole_from:

                def pieces(j):
                    pushed_piece(q, j).wait_send()
                    hop1_piece(q, j).wait_send()

                each(side, pieces)

        each(COLORS, drain)


def factor_of(total, count):
    return jnp.minimum(1.0, 0.5 * lax.rsqrt(jnp.sum(total) / count + 1e-30))


def moments(m, v, g):
    return 0.9 * m + 0.1 * g, 0.95 * v + 0.05 * g * g


def new_weight(w, m, v, g):
    m, v = moments(m, v, g)
    return (w - 0.02 * (m * lax.rsqrt(v + 1e-8) + 0.1 * w)).astype(jnp.bfloat16)


def lanes_of(layers, rows, q, columns, layer):
    per_row = COLORS * columns // 128 * layers
    return [pl.ds((q * columns // 128 + i) * layers + layer, rows, stride=per_row) for i in range(columns // 128)]


def gather_kernel(side, count, *refs):
    total, sums, weights, m, v = refs[0], refs[1:4], refs[4:7], refs[7:10], refs[10:13]
    out, mb, vb = refs[13:16], refs[16:19], refs[19:22]
    gb, wb = refs[22:25], refs[25:28]
    half_w, tmp, lent = refs[28], refs[29], refs[30:32]
    load, swap_s, swap_r, s1, v1, s2, v2, push_s, push_r = refs[32:41]
    s2_piece, v2_piece, piece_s, piece_r = refs[41:45]
    at = Place(side)
    me, core, partner = at.me, at.core, at.partner
    other = 1 - core
    last = side - 1
    down = SLICES - 1

    greet = meet(at)
    sources = [[sums[k], weights[k].at[:, me if k < down else at.chip], m[k], v[k]] for k in range(SLICES)]
    copies = [
        [pltpu.make_async_copy(src, dst[k], load.at[k, i]) for i, (src, dst) in enumerate(zip(sources[k], (gb, wb, mb, vb), strict=True))]
        for k in range(SLICES)
    ]
    for copy in sum(copies, []):
        copy.start()
    greet()
    factor = factor_of(total[...], count)

    def mine(k, layer, q):
        p1, p2, _ = at.way(q)
        return out[k].at[layer, q, p1, p2]

    def swap(k, i, q, layer):
        return remote(lent[k].at[i], mine(k, layer, q), swap_s.at[k, i], swap_r.at[k, i], partner)

    def hop1(k, q, s):
        p1, p2, up = at.way(q)
        ref = out[k].at[core, q, p1, at.moved(p2, -up * s)]
        return remote(ref, ref, s1.at[k, q, s], v1.at[k, q, s], at.next(q, False))

    def hop2(k, q, s):
        p1, _, up = at.way(q)
        ref = out[k].at[core, q, at.moved(p1, -up * s)]
        return remote(ref, ref, s2.at[k, q, s], v2.at[k, q, s], at.next(q, True))

    def push(k, q, s, layer):
        p1, _, up = at.way(q)
        ref = out[k].at[layer, q, at.moved(p1, -up * s)]
        return remote(ref, ref, push_s.at[k, q, s], push_r.at[k, q, s], partner)

    def hop2_piece(q, j):
        p1, _, up = at.way(q)
        ref = out[down].at[core, q, at.moved(p1, -up * (last - 1)), j]
        return remote(ref, ref, s2_piece.at[q, j], v2_piece.at[q, j], at.next(q, True))

    def push_piece(q, j, layer):
        p1, _, up = at.way(q)
        ref = out[down].at[layer, q, at.moved(p1, -up * last), j]
        return remote(ref, ref, piece_s.at[q, j], piece_r.at[q, j], partner)

    def step(k):
        for copy in copies[k]:
            copy.wait()
        for layer in (other, core):
            for i in range(KEPT):
                q = core * KEPT + i
                w = new_weight(wide(wb[k][layer, i]), mb[k][layer, i], vb[k][layer, i], wide(gb[k][layer, i]) * factor)
                if layer is other:
                    lent[k][i] = w
                    swap(k, i, q, other).start()
                else:
                    p1, p2, _ = at.way(q)
                    out[k][layer, q, p1, p2] = w
                    hop1(k, q, 0).start()

    def swapped(k):
        for i in range(KEPT):
            q = other * KEPT + i
            swap(k, i, q, core).wait_recv()
            hop1(k, q, 0).start()

    rows, columns = half_w.shape[-2:]
    half_swap = remote(half_w.at[1], half_w.at[2], swap_s.at[down, 0], swap_r.at[down, 0], partner)

    def step_down(slot):
        for layer in range(CORES):

            @pl.when((layer == core) == (slot == 0))
            def _(layer=layer):
                for q in range(COLORS):
                    tmp[...] = wide(wb[down][layer, :, q * columns : (q + 1) * columns])
                    w = jnp.where(core == 0, tmp[0:rows], tmp[rows : 2 * rows])
                    where = lanes_of(CORES, rows, q, columns, layer)
                    one = jnp.concatenate([mb[down][i, :] for i in where], axis=1)
                    two = jnp.concatenate([vb[down][i, :] for i in where], axis=1)
                    half_w[slot, q] = new_weight(w, one, two, wide(gb[down][layer, q]) * factor)

    def keep_moments(k):
        for layer in range(CORES):
            if k < down:
                for i in range(KEPT):
                    one, two = moments(mb[k][layer, i], vb[k][layer, i], wide(gb[k][layer, i]) * factor)
                    mb[k][layer, i] = one
                    vb[k][layer, i] = two
            else:
                for q in range(COLORS):
                    g = wide(gb[k][layer, q]) * factor
                    for i, where in enumerate(lanes_of(CORES, rows, q, columns, layer)):
                        one, two = moments(mb[k][where, :], vb[k][where, :], g[:, i * 128 : (i + 1) * 128])
                        mb[k][where, :] = one
                        vb[k][where, :] = two

    step(0)
    step(1)
    swapped(0)
    for copy in copies[down]:
        copy.wait()
    step_down(1)
    half_swap.start()
    swapped(1)
    step_down(0)
    half_swap.wait_recv()
    top = 2 * core
    for q in range(COLORS):
        p1, p2, _ = at.way(q)
        tmp[0:rows] = wide(half_w[top, q])
        tmp[rows : 2 * rows] = wide(half_w[2 - top, q])
        out[down][core, q, p1, p2] = tmp[...].astype(jnp.bfloat16)
        hop1(down, q, 0).start()

    for s in range(1, last):
        for k in range(SLICES):

            def first(q):
                hop1(k, q, s - 1).wait_recv()
                hop1(k, q, s).start()

            each(COLORS, first)
    for s in range(side):
        for k in range(SLICES):

            def second(q):
                if s:
                    hop2(k, q, s - 1).wait_recv()
                else:
                    hop1(k, q, last - 1).wait_recv()
                if k == down and s == last - 1:
                    each(side, lambda j: hop2_piece(q, j).start())
                elif s < last:
                    hop2(k, q, s).start()
                push(k, q, s, core).start()

            if k == down and s == last:

                def end(i):
                    j, q = i // COLORS, lax.rem(i, COLORS)
                    hop2_piece(q, j).wait_recv()
                    push_piece(q, j, core).start()

                each(side * COLORS, end)
            else:
                each(COLORS, second)
            if s == 0:
                keep_moments(k)

    for k in range(SLICES):

        def drain(q):
            cut = 1 if k == down else 0
            for s in range(side - cut):
                push(k, q, s, other).wait_recv()
                push(k, q, s, core).wait_send()
            for s in range(last):
                hop1(k, q, s).wait_send()
                if s < last - cut:
                    hop2(k, q, s).wait_send()
            if cut:

                def pieces(j):
                    push_piece(q, j, other).wait_recv()
                    push_piece(q, j, core).wait_send()
                    hop2_piece(q, j).wait_send()

                each(side, pieces)

        each(COLORS, drain)
        if k < down:
            for i in range(KEPT):
                swap(k, i, core * KEPT + i, other).wait_send()
    half_swap.wait_send()


def finish_kernel(side, *refs):
    whole, state, new, new_state, write, store = refs[0:3], refs[3:9], refs[9:12], refs[12:18], refs[18], refs[19]
    for k in range(SLICES):
        for layer in range(CORES):
            for q in range(COLORS):

                def put(t, k=k, layer=layer, q=q):
                    src, dst = whole[k].at[layer, q, t], part(new[k], k, layer, q, t, whole[k].shape[-1])
                    pltpu.make_async_copy(src, dst, write.at[k, layer, q, t]).start()

                each(side, put)
    copies = [pltpu.make_async_copy(src, dst, store.at[i]) for i, (src, dst) in enumerate(zip(state, new_state, strict=True))]
    for copy in copies:
        copy.start()
    for copy in copies:
        copy.wait()
    for k in range(SLICES):
        for layer in range(CORES):

            def wrote(i, k=k, layer=layer):
                q, t = i // side, lax.rem(i, side)
                pltpu.make_async_copy(whole[k].at[layer, q, t], whole[k].at[layer, q, t], write.at[k, layer, q, t]).wait()

            each(COLORS * side, wrote)


def solution(mesh):
    n = mesh.shape["dp"]
    side = math.isqrt(n // CORES)
    bf16, f32 = jnp.bfloat16, jnp.float32
    shape = jax.ShapeDtypeStruct

    def step(*arrays):
        terms, weights, m, v = (arrays[i : i + 3] for i in (0, 3, 6, 9))
        layers, depth, wide_columns = weights[0].shape
        _, deep, columns = weights[2].shape
        chips = side * side
        high, tall = depth // chips // COLORS, deep // chips
        pieces = [(high, wide_columns)] * 2 + [(tall, columns // COLORS)]
        half = (COLORS, tall // CORES, columns // COLORS)
        count = sum(w.size for w in weights)

        views = [t.reshape(layers, side, side, COLORS, high, wide_columns) for t in terms[:2]]
        views.append(terms[2].reshape(layers, side, side, tall, columns))
        kept = [shape((layers, KEPT, high, wide_columns), bf16)] * 2 + [shape((layers, *half), bf16)]
        *sums, total = pl.pallas_call(
            functools.partial(scatter_kernel, side, n),
            name="scatter",
            out_shape=(*kept, shape((8, 128), f32)),
            in_specs=[ANY] * 3,
            out_specs=(ANY,) * 3 + (VMEM,),
            scratch_shapes=[
                *(pltpu.VMEM((COLORS, side, side, *p), bf16) for p in pieces),
                *(pltpu.VMEM((COLORS, side, side, *p), bf16) for p in pieces),
                *(pltpu.VMEM((COLORS, side - 1, side, *p), bf16) for p in pieces),
                *(pltpu.VMEM((COLORS, side - 1, *p), bf16) for p in pieces),
                *(pltpu.VMEM((COLORS, *p), bf16) for p in pieces[:2]),
                pltpu.VMEM((CORES, *half), bf16),
                pltpu.VMEM(pieces[2], f32),
                pltpu.VMEM((n, 8, 128), f32),
                *(DMA((SLICES, COLORS, side)) for _ in range(3)),
                *(DMA((SLICES, COLORS, side - 1)) for _ in range(4)),
                *(DMA((SLICES,)) for _ in range(3)),
                *(DMA((n - 1,)) for _ in range(2)),
                *(DMA((COLORS, side)) for _ in range(4)),
            ],
            compiler_params=pltpu.CompilerParams(collective_id=0, has_side_effects=True, vmem_limit_bytes=ALL_VMEM),
        )(*views)

        def by_lanes(a):
            layers, rows, columns = a.shape
            a = a.transpose(1, 0, 2).reshape(rows, layers, columns // 128, 128)
            return a.transpose(0, 2, 1, 3).reshape(-1, 128)

        def by_rows(a, like):
            layers, rows, columns = like.shape
            a = a.reshape(rows, columns // 128, layers, 128).transpose(0, 2, 1, 3)
            return a.reshape(rows, layers, columns).transpose(1, 0, 2)

        own = [w.reshape(layers, n, KEPT, high, wide_columns) for w in weights[:2]]
        own.append(weights[2].reshape(layers, chips, tall, columns))
        ms, vs = ([a.reshape(layers, KEPT, high, wide_columns) for a in b[:2]] + [by_lanes(b[2])] for b in (m, v))
        state = [pltpu.VMEM(a.shape, f32) for a in ms]
        gathered = pl.pallas_call(
            functools.partial(gather_kernel, side, count),
            name="gather",
            out_shape=(*(pltpu.VMEM((layers, COLORS, side, side, *p), bf16) for p in pieces), *state, *state),
            in_specs=[VMEM] + [ANY] * 12,
            out_specs=(VMEM,) * 9,
            scratch_shapes=[
                *(pltpu.VMEM(k.shape, bf16) for k in kept),
                *(pltpu.VMEM((layers, KEPT, high, wide_columns), bf16) for _ in range(2)),
                pltpu.VMEM((layers, tall, columns), bf16),
                pltpu.VMEM((CORES + 1, *half), bf16),
                pltpu.VMEM(pieces[2], f32),
                *(pltpu.VMEM((KEPT, *p), bf16) for p in pieces[:2]),
                DMA((SLICES, 4)),
                *(DMA((SLICES, KEPT)) for _ in range(2)),
                *(DMA((SLICES, COLORS, side - 1)) for _ in range(4)),
                *(DMA((SLICES, COLORS, side)) for _ in range(2)),
                *(DMA((COLORS, side)) for _ in range(4)),
            ],
            compiler_params=pltpu.CompilerParams(collective_id=1, has_side_effects=True, vmem_limit_bytes=20 << 20),
        )(total, *sums, *own, *ms, *vs)

        gathered = [pltpu.with_memory_space_constraint(a, pltpu.VMEM) for a in gathered]
        outs = pl.pallas_call(
            functools.partial(finish_kernel, side),
            name="finish",
            out_shape=tuple(shape(a.shape, a.dtype) for a in (*[shape(t.shape, bf16) for t in views], *ms, *vs)),
            in_specs=[VMEM] * 9,
            out_specs=(ANY,) * 9,
            scratch_shapes=[DMA((SLICES, CORES, COLORS, side)), DMA((2 * SLICES,))],
            compiler_params=pltpu.CompilerParams(vmem_limit_bytes=20 << 20),
        )(*gathered)
        new = [a.reshape(w.shape) for a, w in zip(outs[:3], weights, strict=True)]
        rest = [
            (by_rows(a, like) if i == SLICES - 1 else a.reshape(like.shape))
            for block in (outs[3:6], outs[6:9])
            for i, (a, like) in enumerate(zip(block, m, strict=True))
        ]
        return (*new, *rest)

    all_of, cut = P(None, None, None), P(None, "dp", None)
    return jax.shard_map(
        step,
        mesh=mesh,
        in_specs=(P(("rep", "dp"), None, None, None),) * 3 + (all_of,) * 3 + (cut,) * 6,
        out_specs=(P("rep", None, None),) * 3 + (P("rep", "dp", None),) * 6,
        check_vma=False,
    )
```

```python
import functools
import math

import jax
import jax.numpy as jnp
from jax import lax
from jax.experimental import pallas as pl
from jax.experimental.pallas import tpu as pltpu
from jax.sharding import PartitionSpec as P

MESH = pl.DeviceIdType.MESH
CORES = 2
COLORS = 4
SLICES = 3
KEPT = COLORS // CORES
ANY = pl.BlockSpec(memory_space=pl.ANY)
VMEM = pl.BlockSpec(memory_space=pltpu.VMEM)
DMA = pltpu.SemaphoreType.DMA


def each(n, body):
    lax.fori_loop(0, n, lambda i, _: body(i), None)


class Place:
    def __init__(self, side):
        self.side = side
        self.me = lax.axis_index("dp")
        self.core = lax.rem(self.me, CORES)
        self.chip = self.me // CORES
        self.x, self.y = self.chip // side, lax.rem(self.chip, side)
        self.partner = self.me + 1 - 2 * self.core

    def at(self, x, y):
        return (x * self.side + y) * CORES + self.core

    def moved(self, p, by):
        return lax.rem(p + by + 2 * self.side, self.side)

    def way(self, q):
        on_x = q < COLORS // 2
        return jnp.where(on_x, self.x, self.y), jnp.where(on_x, self.y, self.x), 1 - 2 * lax.rem(q, 2)

    def next(self, q, first):
        up = 1 - 2 * lax.rem(q, 2)
        on_x = (q < COLORS // 2) == first
        return self.at(jnp.where(on_x, self.moved(self.x, up), self.x), jnp.where(on_x, self.y, self.moved(self.y, up)))


def remote(src, dst, send, recv, device):
    return pltpu.make_async_remote_copy(
        src_ref=src, dst_ref=dst, send_sem=send, recv_sem=recv, device_id={"dp": device}, device_id_type=MESH
    )


def meet(at):
    barrier = pltpu.get_barrier_semaphore()
    near = [at.partner] + [at.next(q, True) for q in range(COLORS)]
    for device in near:
        pl.semaphore_signal(barrier, inc=1, device_id={"dp": device}, device_id_type=MESH)
    return lambda: pl.semaphore_wait(barrier, len(near))


def part(ref, k, layer, q, t, columns):
    if k < SLICES - 1:
        return ref.at[layer, t, :, q] if q < COLORS // 2 else ref.at[layer, :, t, q]
    c = pl.ds(q * columns, columns)
    return ref.at[layer, t, :, :, c] if q < COLORS // 2 else ref.at[layer, :, t, :, c]


def wide(x):
    return x.astype(jnp.float32)


def squares(g):
    total = jnp.zeros((8, 128), jnp.float32)
    for r in range(0, g.shape[0], 8):
        for c in range(0, g.shape[1], 128):
            block = g[r : r + 8, c : c + 128]
            total += block * block
    return total


def factor_of(total, count):
    return jnp.minimum(1.0, 0.5 * lax.rsqrt(jnp.sum(total) / count + 1e-30))


def moments(m, v, g):
    return 0.9 * m + 0.1 * g, 0.95 * v + 0.05 * g * g


def new_weight(w, m, v, g):
    m, v = moments(m, v, g)
    return (w - 0.02 * (m * lax.rsqrt(v + 1e-8) + 0.1 * w)).astype(jnp.bfloat16)


def lanes_of(layers, rows, q, columns, layer):
    per_row = COLORS * columns // 128 * layers
    return [pl.ds((q * columns // 128 + i) * layers + layer, rows, stride=per_row) for i in range(columns // 128)]


def step_kernel(side, n, count, *refs):
    terms, weights, m, v = refs[0:3], refs[3:6], refs[6:9], refs[9:12]
    out, mb, vb = refs[12:15], refs[15:18], refs[18:21]
    r1, r2, fin, lent_sums = refs[21:24], refs[24:27], refs[27:30], refs[30:33]
    half_w, tmp, norms = refs[33:36]
    load, push_s, push_r, state_in = refs[36:40]
    s1, v1, s2, v2 = refs[40:44]
    piece_s, piece_r, s1_piece, v1_piece = refs[44:48]
    norm_s, norm_r, sum_s, sum_r = refs[48:52]
    rows_in, swap_s, swap_r = refs[52:55]
    t1, u1, t2, u2 = refs[55:59]
    give_s, give_r, t2_piece, u2_piece, give_piece_s, give_piece_r = refs[59:65]
    at = Place(side)
    me, core, partner = at.me, at.core, at.partner
    other = 1 - core
    last = side - 1
    down = SLICES - 1
    rows, columns = half_w.shape[-2:]

    def group(q, s):
        p1, _, up = at.way(q)
        return at.moved(p1, -up * (1 + s))

    def loads(k, s):
        for q in range(COLORS):
            t = group(q, s)
            pltpu.make_async_copy(part(terms[k], k, core, q, t, columns), out[k].at[core, q, t], load.at[k, q, s]).start()

    def pushed(k, q, s, src=None):
        dst = out[k].at[core, q, group(q, s)]
        return remote(dst if src is None else src, dst, push_s.at[k, q, s], push_r.at[k, q, s], partner)

    def pushes(k, s):
        for q in range(COLORS):
            pushed(k, q, s, part(terms[k], k, other, q, group(q, s), columns)).start()

    def loaded(k, q, s):
        ref = out[k].at[core, q, group(q, s)]
        pltpu.make_async_copy(ref, ref, load.at[k, q, s]).wait()

    def ready(k, q, s):
        loaded(k, q, s)
        pushed(k, q, s).wait_recv()

    def pushed_piece(q, j, src=None):
        dst = out[0].at[core, q, group(q, 0), j]
        return remote(dst if src is None else src, dst, piece_s.at[q, j], piece_r.at[q, j], partner)

    def sum1_piece(q, j):
        src = out[0].at[core, q, group(q, 0), j]
        return remote(src, r1[0].at[q, 0, j], s1_piece.at[q, j], v1_piece.at[q, j], at.next(q, True))

    def sum1(k, q, s):
        src = r1[k].at[q, s - 1] if s else out[k].at[core, q, group(q, s)]
        return remote(src, r1[k].at[q, s], s1.at[k, q, s], v1.at[k, q, s], at.next(q, True))

    def sum2(k, q, s):
        _, p2, up = at.way(q)
        src = r2[k].at[q, s - 1] if s else r1[k].at[q, last - 1, at.moved(p2, -up)]
        return remote(src, r2[k].at[q, s], s2.at[k, q, s], v2.at[k, q, s], at.next(q, False))

    greet = meet(at)
    for k in range(SLICES):
        loads(k, 0)
    greet()
    for j in range(side):
        for q in range(COLORS):
            pushed_piece(q, j, part(terms[0], 0, other, q, group(q, 0), columns).at[j]).start()
    for k in range(1, SLICES):
        pushes(k, 0)

    def both(k, q, t, j):
        return wide(out[k][0, q, t, j]) + wide(out[k][1, q, t, j])

    for j in range(side):

        def start(q):
            t = group(q, 0)
            if j == 0:
                loaded(0, q, 0)
            pushed_piece(q, j).wait_recv()
            out[0][core, q, t, j] = both(0, q, t, j).astype(jnp.bfloat16)
            sum1_piece(q, j).start()

        each(COLORS, start)
    loads(0, 1)
    pushes(0, 1)
    for s in range(last):
        for k in range(SLICES):
            if s == 0 and k == 0:
                continue

            def first(q):
                t = group(q, s)
                if s == 1 and k == 0:
                    each(side, lambda j: sum1_piece(q, j).wait_recv())
                elif s:
                    sum1(k, q, s - 1).wait_recv()
                ready(k, q, s)

                def add(j):
                    if s:
                        r1[k][q, s - 1, j] = (wide(r1[k][q, s - 1, j]) + both(k, q, t, j)).astype(jnp.bfloat16)
                    else:
                        out[k][core, q, t, j] = both(k, q, t, j).astype(jnp.bfloat16)

                each(side, add)
                sum1(k, q, s).start()

            each(COLORS, first)
            loads(k, s + 1)
            pushes(k, s + 1)
        if s == 0:
            moments_in = [
                pltpu.make_async_copy(src[k], dst[k], state_in.at[k, i])
                for k in range(SLICES)
                for i, (src, dst) in enumerate(((m, mb), (v, vb)))
            ]
            for copy in moments_in:
                copy.start()

    def here(k, q, u):
        p1, _, _ = at.way(q)
        return both(k, q, p1, u) + wide(r1[k][q, last - 1, u])

    for s in range(last):
        for k in range(SLICES):

            def second(q):
                _, p2, up = at.way(q)
                u = at.moved(p2, -up * (1 + s))
                if s:
                    sum2(k, q, s - 1).wait_recv()
                    r2[k][q, s - 1] = (wide(r2[k][q, s - 1]) + here(k, q, u)).astype(jnp.bfloat16)
                else:
                    sum1(k, q, last - 1).wait_recv()
                    ready(k, q, last)
                    r1[k][q, last - 1, u] = here(k, q, u).astype(jnp.bfloat16)
                sum2(k, q, s).start()

            each(COLORS, second)

    def share(k, of):
        return fin[k].at[pl.ds(of * KEPT, KEPT)] if k < down else fin[k].at[of]

    def swap_sums(k):
        return remote(share(k, other), lent_sums[k], sum_s.at[k], sum_r.at[k], partner)

    def norm(i):
        return remote(norms.at[me], norms.at[me], norm_s.at[i], norm_r.at[i], lax.rem(me + 1 + i, n))

    norms[me] = jnp.zeros((8, 128), jnp.float32)
    for k in range(SLICES):

        def end(q):
            _, p2, _ = at.way(q)
            sum2(k, q, last - 1).wait_recv()
            g = (wide(r2[k][q, last - 1]) + here(k, q, p2)).astype(jnp.bfloat16)
            norms[me] += squares(wide(g))
            if k < down:
                fin[k][q] = g
            else:
                tmp[...] = wide(g)
                for h in range(CORES):
                    fin[k][h, q] = tmp[h * rows : (h + 1) * rows].astype(jnp.bfloat16)

            if k:
                sum1(k, q, 0).wait_send()
            else:
                each(side, lambda j: sum1_piece(q, j).wait_send())

        each(COLORS, end)
        if k < down:
            swap_sums(k).start()
    each(n - 1, lambda i: norm(i).start())
    swap_sums(down).start()
    for k in range(SLICES):

        def drain(q):
            for s in range(side):
                if k or s:
                    pushed(k, q, s).wait_send()
            for s in range(last):
                if s:
                    sum1(k, q, s).wait_send()
                sum2(k, q, s).wait_send()
            if k == 0:
                each(side, lambda j: pushed_piece(q, j).wait_send())

        each(COLORS, drain)

    def old(k, layer, i):
        return r1[k].at[0, 0, layer * KEPT + i] if k < down else r1[k].at[layer, 0, i]

    def rows_of(k):
        for layer in range(CORES):
            for i in range(KEPT if k < down else COLORS):
                if k < down:
                    src = weights[k].at[layer, me, i]
                else:
                    src = weights[k].at[layer, at.chip, :, pl.ds(i * columns, columns)]
                yield pltpu.make_async_copy(src, old(k, layer, i), rows_in.at[k, layer, i])

    for k in range(SLICES):
        for copy in rows_of(k):
            copy.start()
    for copy in moments_in:
        copy.wait()
    for k in range(SLICES):
        swap_sums(k).wait_recv()
        for copy in rows_of(k):
            copy.wait()
    each(n - 1, lambda i: norm(i).wait_recv())
    tmp[0:8, 0:128] = jnp.zeros((8, 128), jnp.float32)

    def tally(i):
        tmp[0:8, 0:128] += norms[i]

    each(n, tally)
    factor = factor_of(tmp[0:8, 0:128], count)

    def swap(k, i, q, layer):
        p1, p2, _ = at.way(q)
        return remote(r2[k].at[i, 0], out[k].at[layer, q, p1, p2], swap_s.at[k, i], swap_r.at[k, i], partner)

    def hop1(k, q, s):
        p1, p2, up = at.way(q)
        ref = out[k].at[core, q, p1, at.moved(p2, -up * s)]
        return remote(ref, ref, t1.at[k, q, s], u1.at[k, q, s], at.next(q, False))

    def hop2(k, q, s):
        p1, _, up = at.way(q)
        ref = out[k].at[core, q, at.moved(p1, -up * s)]
        return remote(ref, ref, t2.at[k, q, s], u2.at[k, q, s], at.next(q, True))

    def give(k, q, s, layer):
        p1, _, up = at.way(q)
        ref = out[k].at[layer, q, at.moved(p1, -up * s)]
        return remote(ref, ref, give_s.at[k, q, s], give_r.at[k, q, s], partner)

    def hop2_piece(q, j):
        p1, _, up = at.way(q)
        ref = out[down].at[core, q, at.moved(p1, -up * (last - 1)), j]
        return remote(ref, ref, t2_piece.at[q, j], u2_piece.at[q, j], at.next(q, True))

    def give_piece(q, j, layer):
        p1, _, up = at.way(q)
        ref = out[down].at[layer, q, at.moved(p1, -up * last), j]
        return remote(ref, ref, give_piece_s.at[q, j], give_piece_r.at[q, j], partner)

    def gradient(k, mine, i):
        if k < down:
            return wide(fin[k][core * KEPT + i] if mine else lent_sums[k][i]) * factor
        return wide(fin[k][core, i] if mine else lent_sums[k][i]) * factor

    def step(k):
        for layer, mine in ((core, True), (other, False)):
            for i in range(KEPT):
                q = core * KEPT + i
                w = new_weight(wide(old(k, layer, i)[...]), mb[k][layer, i], vb[k][layer, i], gradient(k, mine, i))
                if mine:
                    p1, p2, _ = at.way(q)
                    out[k][layer, q, p1, p2] = w
                    hop1(k, q, 0).start()
                else:
                    r2[k][i, 0] = w
                    swap(k, i, q, other).start()

    def swapped(k):
        for i in range(KEPT):
            q = other * KEPT + i
            swap(k, i, q, core).wait_recv()
            hop1(k, q, 0).start()

    half_swap = remote(fin[down].at[other], half_w.at[1], swap_s.at[down, 0], swap_r.at[down, 0], partner)

    def for_layer(mine, body):
        for layer in range(CORES):
            pl.when((layer == core) == mine)(functools.partial(body, layer))

    def step_down(mine):
        def body(layer):
            for q in range(COLORS):
                tmp[...] = wide(old(down, layer, q)[...])
                w = jnp.where(core == 0, tmp[0:rows], tmp[rows : 2 * rows])
                where = lanes_of(CORES, rows, q, columns, layer)
                one = jnp.concatenate([mb[down][i, :] for i in where], axis=1)
                two = jnp.concatenate([vb[down][i, :] for i in where], axis=1)
                w = new_weight(w, one, two, gradient(down, mine, q))
                if mine:
                    half_w[0, q] = w
                else:
                    fin[down][other, q] = w

        for_layer(mine, body)

    def keep_moments(k):
        for mine in (True, False):
            if k < down:
                layer = core if mine else other
                for i in range(KEPT):
                    one, two = moments(mb[k][layer, i], vb[k][layer, i], gradient(k, mine, i))
                    mb[k][layer, i] = one
                    vb[k][layer, i] = two
                continue

            def body(layer, mine=mine):
                for q in range(COLORS):
                    g = gradient(down, mine, q)
                    for i, where in enumerate(lanes_of(CORES, rows, q, columns, layer)):
                        one, two = moments(mb[k][where, :], vb[k][where, :], g[:, i * 128 : (i + 1) * 128])
                        mb[k][where, :] = one
                        vb[k][where, :] = two

            for_layer(mine, body)

    step(0)
    step(1)
    swapped(0)
    swap_sums(down).wait_send()
    step_down(False)
    half_swap.start()
    swapped(1)
    step_down(True)
    half_swap.wait_recv()
    for q in range(COLORS):
        p1, p2, _ = at.way(q)
        tmp[0:rows] = wide(half_w[core, q])
        tmp[rows : 2 * rows] = wide(half_w[other, q])
        out[down][core, q, p1, p2] = tmp[...].astype(jnp.bfloat16)
        hop1(down, q, 0).start()

    for s in range(1, last):
        for k in range(SLICES):

            def spread(q):
                hop1(k, q, s - 1).wait_recv()
                hop1(k, q, s).start()

            each(COLORS, spread)
    for s in range(side):
        for k in range(SLICES):

            def onward(q):
                if s:
                    hop2(k, q, s - 1).wait_recv()
                else:
                    hop1(k, q, last - 1).wait_recv()
                if k == down and s == last - 1:
                    each(side, lambda j: hop2_piece(q, j).start())
                elif s < last:
                    hop2(k, q, s).start()
                give(k, q, s, core).start()

            def onward_piece(i):
                j, q = i // COLORS, lax.rem(i, COLORS)
                hop2_piece(q, j).wait_recv()
                give_piece(q, j, core).start()

            if k == down and s == last:
                each(side * COLORS, onward_piece)
            else:
                each(COLORS, onward)
            if s == 0:
                keep_moments(k)

    for k in range(SLICES):

        def settle(q):
            cut = 1 if k == down else 0
            for s in range(side - cut):
                give(k, q, s, other).wait_recv()
                give(k, q, s, core).wait_send()
            for s in range(last):
                hop1(k, q, s).wait_send()
                if s < last - cut:
                    hop2(k, q, s).wait_send()
            if cut:

                def pieces(j):
                    give_piece(q, j, other).wait_recv()
                    give_piece(q, j, core).wait_send()
                    hop2_piece(q, j).wait_send()

                each(side, pieces)

        each(COLORS, settle)
        if k < down:
            swap_sums(k).wait_send()
            for i in range(KEPT):
                swap(k, i, core * KEPT + i, other).wait_send()
    half_swap.wait_send()
    each(n - 1, lambda i: norm(i).wait_send())


def finish_kernel(side, *refs):
    whole, state, new, new_state, write, store = refs[0:3], refs[3:9], refs[9:12], refs[12:18], refs[18], refs[19]
    for k in range(SLICES):
        for layer in range(CORES):
            for q in range(COLORS):

                def put(t, k=k, layer=layer, q=q):
                    src, dst = whole[k].at[layer, q, t], part(new[k], k, layer, q, t, whole[k].shape[-1])
                    pltpu.make_async_copy(src, dst, write.at[k, layer, q, t]).start()

                each(side, put)
    copies = [pltpu.make_async_copy(src, dst, store.at[i]) for i, (src, dst) in enumerate(zip(state, new_state, strict=True))]
    for copy in copies:
        copy.start()
    for copy in copies:
        copy.wait()
    for k in range(SLICES):
        for layer in range(CORES):

            def wrote(i, k=k, layer=layer):
                q, t = i // side, lax.rem(i, side)
                pltpu.make_async_copy(whole[k].at[layer, q, t], whole[k].at[layer, q, t], write.at[k, layer, q, t]).wait()

            each(COLORS * side, wrote)


def solution(mesh):
    n = mesh.shape["dp"]
    side = math.isqrt(n // CORES)
    bf16, f32 = jnp.bfloat16, jnp.float32
    shape = jax.ShapeDtypeStruct

    def step(*arrays):
        terms, weights, m, v = (arrays[i : i + 3] for i in (0, 3, 6, 9))
        layers, depth, wide_columns = weights[0].shape
        _, deep, columns = weights[2].shape
        chips = side * side
        high, tall = depth // chips // COLORS, deep // chips
        pieces = [(high, wide_columns)] * 2 + [(tall, columns // COLORS)]
        half = (COLORS, tall // CORES, columns // COLORS)
        count = sum(w.size for w in weights)

        views = [t.reshape(layers, side, side, COLORS, high, wide_columns) for t in terms[:2]]
        views.append(terms[2].reshape(layers, side, side, tall, columns))
        def by_lanes(a):
            layers, rows, columns = a.shape
            a = a.transpose(1, 0, 2).reshape(rows, layers, columns // 128, 128)
            return a.transpose(0, 2, 1, 3).reshape(-1, 128)

        def by_rows(a, like):
            layers, rows, columns = like.shape
            a = a.reshape(rows, columns // 128, layers, 128).transpose(0, 2, 1, 3)
            return a.reshape(rows, layers, columns).transpose(1, 0, 2)

        own = [w.reshape(layers, n, KEPT, high, wide_columns) for w in weights[:2]]
        own.append(weights[2].reshape(layers, chips, tall, columns))
        ms, vs = ([a.reshape(layers, KEPT, high, wide_columns) for a in b[:2]] + [by_lanes(b[2])] for b in (m, v))
        state = [pltpu.VMEM(a.shape, f32) for a in ms]
        gathered = pl.pallas_call(
            functools.partial(step_kernel, side, n, count),
            name="step",
            out_shape=(*(pltpu.VMEM((layers, COLORS, side, side, *p), bf16) for p in pieces), *state, *state),
            in_specs=[ANY] * 12,
            out_specs=(VMEM,) * 9,
            scratch_shapes=[
                *(pltpu.VMEM((COLORS, side - 1, side, *p), bf16) for p in pieces),
                *(pltpu.VMEM((COLORS, side - 1, *p), bf16) for p in pieces),
                *(pltpu.VMEM((COLORS, *p), bf16) for p in pieces[:2]),
                pltpu.VMEM((CORES, *half), bf16),
                *(pltpu.VMEM((KEPT, *p), bf16) for p in pieces[:2]),
                pltpu.VMEM(half, bf16),
                pltpu.VMEM((CORES, *half), bf16),
                pltpu.VMEM(pieces[2], f32),
                pltpu.VMEM((n, 8, 128), f32),
                *(DMA((SLICES, COLORS, side)) for _ in range(3)),
                DMA((SLICES, 2)),
                *(DMA((SLICES, COLORS, side - 1)) for _ in range(4)),
                *(DMA((COLORS, side)) for _ in range(4)),
                *(DMA((n - 1,)) for _ in range(2)),
                *(DMA((SLICES,)) for _ in range(2)),
                DMA((SLICES, CORES, COLORS)),
                *(DMA((SLICES, KEPT)) for _ in range(2)),
                *(DMA((SLICES, COLORS, side - 1)) for _ in range(4)),
                *(DMA((SLICES, COLORS, side)) for _ in range(2)),
                *(DMA((COLORS, side)) for _ in range(4)),
            ],
            compiler_params=pltpu.CompilerParams(collective_id=0, has_side_effects=True, vmem_limit_bytes=22_806_528),
        )(*views, *own, *ms, *vs)
        gathered = [pltpu.with_memory_space_constraint(a, pltpu.VMEM) for a in gathered]
        outs = pl.pallas_call(
            functools.partial(finish_kernel, side),
            name="finish",
            out_shape=tuple(shape(a.shape, a.dtype) for a in (*[shape(t.shape, bf16) for t in views], *ms, *vs)),
            in_specs=[VMEM] * 9,
            out_specs=(ANY,) * 9,
            scratch_shapes=[DMA((SLICES, CORES, COLORS, side)), DMA((2 * SLICES,))],
            compiler_params=pltpu.CompilerParams(vmem_limit_bytes=22_806_528),
        )(*gathered)
        new = [a.reshape(w.shape) for a, w in zip(outs[:3], weights, strict=True)]
        rest = [
            (by_rows(a, like) if i == SLICES - 1 else a.reshape(like.shape))
            for block in (outs[3:6], outs[6:9])
            for i, (a, like) in enumerate(zip(block, m, strict=True))
        ]
        return (*new, *rest)

    all_of, cut = P(None, None, None), P(None, "dp", None)
    return jax.shard_map(
        step,
        mesh=mesh,
        in_specs=(P(("rep", "dp"), None, None, None),) * 3 + (all_of,) * 3 + (cut,) * 6,
        out_specs=(P("rep", None, None),) * 3 + (P("rep", "dp", None),) * 6,
        check_vma=False,
    )
```

```python
import functools
import math

import jax
import jax.numpy as jnp
from jax import lax
from jax.experimental import pallas as pl
from jax.experimental.pallas import tpu as pltpu
from jax.sharding import PartitionSpec as P

MESH = pl.DeviceIdType.MESH
CORES = 2
COLORS = 4
SLICES = 3
KEPT = COLORS // CORES
ANY = pl.BlockSpec(memory_space=pl.ANY)
VMEM = pl.BlockSpec(memory_space=pltpu.VMEM)
DMA = pltpu.SemaphoreType.DMA


def each(n, body):
    lax.fori_loop(0, n, lambda i, _: body(i), None)


class Place:
    def __init__(self, side):
        self.side = side
        self.me = lax.axis_index("dp")
        self.core = lax.rem(self.me, CORES)
        self.chip = self.me // CORES
        self.x, self.y = self.chip // side, lax.rem(self.chip, side)
        self.partner = self.me + 1 - 2 * self.core

    def at(self, x, y):
        return (x * self.side + y) * CORES + self.core

    def moved(self, p, by):
        return lax.rem(p + by + 2 * self.side, self.side)

    def way(self, q):
        on_x = q < COLORS // 2
        return jnp.where(on_x, self.x, self.y), jnp.where(on_x, self.y, self.x), 1 - 2 * lax.rem(q, 2)

    def next(self, q, first):
        up = 1 - 2 * lax.rem(q, 2)
        on_x = (q < COLORS // 2) == first
        return self.at(jnp.where(on_x, self.moved(self.x, up), self.x), jnp.where(on_x, self.y, self.moved(self.y, up)))


def remote(src, dst, send, recv, device):
    return pltpu.make_async_remote_copy(
        src_ref=src, dst_ref=dst, send_sem=send, recv_sem=recv, device_id={"dp": device}, device_id_type=MESH
    )


def meet(at):
    barrier = pltpu.get_barrier_semaphore()
    near = [at.partner] + [at.next(q, True) for q in range(COLORS)]
    for device in near:
        pl.semaphore_signal(barrier, inc=1, device_id={"dp": device}, device_id_type=MESH)
    return lambda: pl.semaphore_wait(barrier, len(near))


def part(ref, k, layer, q, t, columns):
    if k < SLICES - 1:
        return ref.at[layer, t, :, q] if q < COLORS // 2 else ref.at[layer, :, t, q]
    c = pl.ds(q * columns, columns)
    return ref.at[layer, t, :, :, c] if q < COLORS // 2 else ref.at[layer, :, t, :, c]


def wide(x):
    return x.astype(jnp.float32)


def squares(g):
    total = jnp.zeros((8, 128), jnp.float32)
    for r in range(0, g.shape[0], 8):
        for c in range(0, g.shape[1], 128):
            block = g[r : r + 8, c : c + 128]
            total += block * block
    return total


def factor_of(total, count):
    return jnp.minimum(1.0, 0.5 * lax.rsqrt(jnp.sum(total) / count + 1e-30))


def moments(m, v, g):
    return 0.9 * m + 0.1 * g, 0.95 * v + 0.05 * g * g


def new_weight(w, m, v, g):
    m, v = moments(m, v, g)
    return (w - 0.02 * (m * lax.rsqrt(v + 1e-8) + 0.1 * w)).astype(jnp.bfloat16)


def lanes_of(layers, rows, q, columns, layer):
    per_row = COLORS * columns // 128 * layers
    return [pl.ds((q * columns // 128 + i) * layers + layer, rows, stride=per_row) for i in range(columns // 128)]


def step_kernel(side, n, count, *refs):
    terms, weights, m, v = refs[0:3], refs[3:6], refs[6:9], refs[9:12]
    out, mb, vb = refs[12:15], refs[15:18], refs[18:21]
    r1, r2, fin, lent_sums = refs[21:24], refs[24:27], refs[27:30], refs[30:33]
    half_w, tmp, norms = refs[33:36]
    load, push_s, push_r, state_in = refs[36:40]
    s1, v1, s2, v2 = refs[40:44]
    piece_s, piece_r, s1_piece, v1_piece = refs[44:48]
    norm_s, norm_r, sum_s, sum_r = refs[48:52]
    rows_in, swap_s, swap_r = refs[52:55]
    t1, u1, t2, u2 = refs[55:59]
    give_s, give_r, t2_piece, u2_piece, give_piece_s, give_piece_r = refs[59:65]
    at = Place(side)
    me, core, partner = at.me, at.core, at.partner
    other = 1 - core
    last = side - 1
    down = SLICES - 1
    rows, columns = half_w.shape[-2:]

    def group(q, s):
        p1, _, up = at.way(q)
        return at.moved(p1, -up * (1 + s))

    def loads(k, s):
        for q in range(COLORS):
            t = group(q, s)
            pltpu.make_async_copy(part(terms[k], k, core, q, t, columns), out[k].at[core, q, t], load.at[k, q, s]).start()

    def pushed(k, q, s, src=None):
        dst = out[k].at[core, q, group(q, s)]
        return remote(dst if src is None else src, dst, push_s.at[k, q, s], push_r.at[k, q, s], partner)

    def pushes(k, s):
        for q in range(COLORS):
            pushed(k, q, s, part(terms[k], k, other, q, group(q, s), columns)).start()

    def loaded(k, q, s):
        ref = out[k].at[core, q, group(q, s)]
        pltpu.make_async_copy(ref, ref, load.at[k, q, s]).wait()

    def ready(k, q, s):
        loaded(k, q, s)
        pushed(k, q, s).wait_recv()

    def pushed_piece(q, j, src=None):
        dst = out[0].at[core, q, group(q, 0), j]
        return remote(dst if src is None else src, dst, piece_s.at[q, j], piece_r.at[q, j], partner)

    def sum1_piece(q, j):
        src = out[0].at[core, q, group(q, 0), j]
        return remote(src, r1[0].at[q, 0, j], s1_piece.at[q, j], v1_piece.at[q, j], at.next(q, True))

    def sum1(k, q, s):
        src = r1[k].at[q, s - 1] if s else out[k].at[core, q, group(q, s)]
        return remote(src, r1[k].at[q, s], s1.at[k, q, s], v1.at[k, q, s], at.next(q, True))

    def sum2(k, q, s):
        _, p2, up = at.way(q)
        src = r2[k].at[q, s - 1] if s else r1[k].at[q, last - 1, at.moved(p2, -up)]
        return remote(src, r2[k].at[q, s], s2.at[k, q, s], v2.at[k, q, s], at.next(q, False))

    greet = meet(at)
    for k in range(SLICES):
        loads(k, 0)
    greet()
    for j in range(side):
        for q in range(COLORS):
            pushed_piece(q, j, part(terms[0], 0, other, q, group(q, 0), columns).at[j]).start()
    for k in range(1, SLICES):
        pushes(k, 0)

    def both(k, q, t, j):
        return wide(out[k][0, q, t, j]) + wide(out[k][1, q, t, j])

    for j in range(side):

        def start(q):
            t = group(q, 0)
            if j == 0:
                loaded(0, q, 0)
            pushed_piece(q, j).wait_recv()
            out[0][core, q, t, j] = both(0, q, t, j).astype(jnp.bfloat16)
            sum1_piece(q, j).start()

        each(COLORS, start)
    loads(0, 1)
    pushes(0, 1)
    for s in range(last):
        for k in range(SLICES):
            if s == 0 and k == 0:
                continue

            def first(q):
                t = group(q, s)
                if s == 1 and k == 0:
                    each(side, lambda j: sum1_piece(q, j).wait_recv())
                elif s:
                    sum1(k, q, s - 1).wait_recv()
                ready(k, q, s)

                def add(j):
                    if s:
                        r1[k][q, s - 1, j] = (wide(r1[k][q, s - 1, j]) + both(k, q, t, j)).astype(jnp.bfloat16)
                    else:
                        out[k][core, q, t, j] = both(k, q, t, j).astype(jnp.bfloat16)

                each(side, add)
                sum1(k, q, s).start()

            each(COLORS, first)
            loads(k, s + 1)
            pushes(k, s + 1)
        if s == 0:
            moments_in = [
                pltpu.make_async_copy(src[k], dst[k], state_in.at[k, i])
                for k in range(SLICES)
                for i, (src, dst) in enumerate(((m, mb), (v, vb)))
            ]
            for copy in moments_in:
                copy.start()

    def here(k, q, u):
        p1, _, _ = at.way(q)
        return both(k, q, p1, u) + wide(r1[k][q, last - 1, u])

    for s in range(last):
        for k in range(SLICES):

            def second(q):
                _, p2, up = at.way(q)
                u = at.moved(p2, -up * (1 + s))
                if s:
                    sum2(k, q, s - 1).wait_recv()
                    r2[k][q, s - 1] = (wide(r2[k][q, s - 1]) + here(k, q, u)).astype(jnp.bfloat16)
                else:
                    sum1(k, q, last - 1).wait_recv()
                    ready(k, q, last)
                    r1[k][q, last - 1, u] = here(k, q, u).astype(jnp.bfloat16)
                sum2(k, q, s).start()

            each(COLORS, second)

    def share(k, of):
        return fin[k].at[pl.ds(of * KEPT, KEPT)] if k < down else fin[k].at[of]

    def swap_sums(k):
        return remote(share(k, other), lent_sums[k], sum_s.at[k], sum_r.at[k], partner)

    def norm(i):
        return remote(norms.at[me], norms.at[me], norm_s.at[i], norm_r.at[i], lax.rem(me + 1 + i, n))

    norms[me] = jnp.zeros((8, 128), jnp.float32)
    for k in range(SLICES):

        def end(q):
            _, p2, _ = at.way(q)
            sum2(k, q, last - 1).wait_recv()
            g = (wide(r2[k][q, last - 1]) + here(k, q, p2)).astype(jnp.bfloat16)
            norms[me] += squares(wide(g))
            if k < down:
                fin[k][q] = g
            else:
                r2[k][q, last - 1] = g

            if k:
                sum1(k, q, 0).wait_send()
            else:
                each(side, lambda j: sum1_piece(q, j).wait_send())

        each(COLORS, end)
        if k < down:
            swap_sums(k).start()
    each(n - 1, lambda i: norm(i).start())

    def halve(q):
        tmp[...] = wide(r2[down][q, last - 1])
        for h in range(CORES):
            fin[down][h, q] = tmp[h * rows : (h + 1) * rows].astype(jnp.bfloat16)

    each(COLORS, halve)
    swap_sums(down).start()
    for k in range(SLICES):

        def drain(q):
            for s in range(side):
                if k or s:
                    pushed(k, q, s).wait_send()
            for s in range(last):
                if s:
                    sum1(k, q, s).wait_send()
                sum2(k, q, s).wait_send()
            if k == 0:
                each(side, lambda j: pushed_piece(q, j).wait_send())

        each(COLORS, drain)

    def old(k, layer, i):
        return r1[k].at[0, 0, layer * KEPT + i] if k < down else r1[k].at[layer, 0, i]

    def rows_of(k):
        for layer in range(CORES):
            for i in range(KEPT if k < down else COLORS):
                if k < down:
                    src = weights[k].at[layer, me, i]
                else:
                    src = weights[k].at[layer, at.chip, :, pl.ds(i * columns, columns)]
                yield pltpu.make_async_copy(src, old(k, layer, i), rows_in.at[k, layer, i])

    for k in range(SLICES):
        for copy in rows_of(k):
            copy.start()
    for copy in moments_in:
        copy.wait()
    for k in range(SLICES):
        swap_sums(k).wait_recv()
        for copy in rows_of(k):
            copy.wait()
    each(n - 1, lambda i: norm(i).wait_recv())
    factor = factor_of(jnp.sum(norms[...], axis=0), count)

    def swap(k, i, q, layer):
        p1, p2, _ = at.way(q)
        return remote(r2[k].at[i, 0], out[k].at[layer, q, p1, p2], swap_s.at[k, i], swap_r.at[k, i], partner)

    def hop1(k, q, s):
        p1, p2, up = at.way(q)
        ref = out[k].at[core, q, p1, at.moved(p2, -up * s)]
        return remote(ref, ref, t1.at[k, q, s], u1.at[k, q, s], at.next(q, False))

    def hop2(k, q, s):
        p1, _, up = at.way(q)
        ref = out[k].at[core, q, at.moved(p1, -up * s)]
        return remote(ref, ref, t2.at[k, q, s], u2.at[k, q, s], at.next(q, True))

    def give(k, q, s, layer):
        p1, _, up = at.way(q)
        ref = out[k].at[layer, q, at.moved(p1, -up * s)]
        return remote(ref, ref, give_s.at[k, q, s], give_r.at[k, q, s], partner)

    def hop2_piece(q, j):
        p1, _, up = at.way(q)
        ref = out[down].at[core, q, at.moved(p1, -up * (last - 1)), j]
        return remote(ref, ref, t2_piece.at[q, j], u2_piece.at[q, j], at.next(q, True))

    def give_piece(q, j, layer):
        p1, _, up = at.way(q)
        ref = out[down].at[layer, q, at.moved(p1, -up * last), j]
        return remote(ref, ref, give_piece_s.at[q, j], give_piece_r.at[q, j], partner)

    def gradient(k, mine, i):
        if k < down:
            return wide(fin[k][core * KEPT + i] if mine else lent_sums[k][i]) * factor
        return wide(fin[k][core, i] if mine else lent_sums[k][i]) * factor

    def step(k):
        for layer, mine in ((core, True), (other, False)):
            for i in range(KEPT):
                q = core * KEPT + i
                w = new_weight(wide(old(k, layer, i)[...]), mb[k][layer, i], vb[k][layer, i], gradient(k, mine, i))
                if mine:
                    p1, p2, _ = at.way(q)
                    out[k][layer, q, p1, p2] = w
                    hop1(k, q, 0).start()
                else:
                    r2[k][i, 0] = w
                    swap(k, i, q, other).start()

    def swapped(k):
        for i in range(KEPT):
            q = other * KEPT + i
            swap(k, i, q, core).wait_recv()
            hop1(k, q, 0).start()

    half_swap = remote(fin[down].at[other], half_w.at[1], swap_s.at[down, 0], swap_r.at[down, 0], partner)

    def for_layer(mine, body):
        for layer in range(CORES):
            pl.when((layer == core) == mine)(functools.partial(body, layer))

    def step_down(mine):
        def body(layer):
            for q in range(COLORS):
                tmp[...] = wide(old(down, layer, q)[...])
                w = jnp.where(core == 0, tmp[0:rows], tmp[rows : 2 * rows])
                where = lanes_of(CORES, rows, q, columns, layer)
                one = jnp.concatenate([mb[down][i, :] for i in where], axis=1)
                two = jnp.concatenate([vb[down][i, :] for i in where], axis=1)
                w = new_weight(w, one, two, gradient(down, mine, q))
                if mine:
                    half_w[0, q] = w
                else:
                    fin[down][other, q] = w

        for_layer(mine, body)

    def keep_moments(k):
        for mine in (True, False):
            if k < down:
                layer = core if mine else other
                for i in range(KEPT):
                    one, two = moments(mb[k][layer, i], vb[k][layer, i], gradient(k, mine, i))
                    mb[k][layer, i] = one
                    vb[k][layer, i] = two
                continue

            def body(layer, mine=mine):
                for q in range(COLORS):
                    g = gradient(down, mine, q)
                    for i, where in enumerate(lanes_of(CORES, rows, q, columns, layer)):
                        one, two = moments(mb[k][where, :], vb[k][where, :], g[:, i * 128 : (i + 1) * 128])
                        mb[k][where, :] = one
                        vb[k][where, :] = two

            for_layer(mine, body)

    step(0)
    step(1)
    swapped(0)
    swap_sums(down).wait_send()
    step_down(False)
    half_swap.start()
    swapped(1)
    step_down(True)
    half_swap.wait_recv()
    for q in range(COLORS):
        p1, p2, _ = at.way(q)
        tmp[0:rows] = wide(half_w[core, q])
        tmp[rows : 2 * rows] = wide(half_w[other, q])
        out[down][core, q, p1, p2] = tmp[...].astype(jnp.bfloat16)
        hop1(down, q, 0).start()

    for s in range(1, last):
        for k in range(SLICES):

            def spread(q):
                hop1(k, q, s - 1).wait_recv()
                hop1(k, q, s).start()

            each(COLORS, spread)
    for s in range(side):
        for k in range(SLICES):

            def onward(q):
                if s:
                    hop2(k, q, s - 1).wait_recv()
                else:
                    hop1(k, q, last - 1).wait_recv()
                if k == down and s == last - 1:
                    each(side, lambda j: hop2_piece(q, j).start())
                elif s < last:
                    hop2(k, q, s).start()
                give(k, q, s, core).start()

            def onward_piece(i):
                j, q = i // COLORS, lax.rem(i, COLORS)
                hop2_piece(q, j).wait_recv()
                give_piece(q, j, core).start()

            if k == down and s == last:
                each(side * COLORS, onward_piece)
            else:
                each(COLORS, onward)
            if s == 0:
                keep_moments(k)

    for k in range(SLICES):

        def settle(q):
            cut = 1 if k == down else 0
            for s in range(side - cut):
                give(k, q, s, other).wait_recv()
                give(k, q, s, core).wait_send()
            for s in range(last):
                hop1(k, q, s).wait_send()
                if s < last - cut:
                    hop2(k, q, s).wait_send()
            if cut:

                def pieces(j):
                    give_piece(q, j, other).wait_recv()
                    give_piece(q, j, core).wait_send()
                    hop2_piece(q, j).wait_send()

                each(side, pieces)

        each(COLORS, settle)
        if k < down:
            swap_sums(k).wait_send()
            for i in range(KEPT):
                swap(k, i, core * KEPT + i, other).wait_send()
    half_swap.wait_send()
    each(n - 1, lambda i: norm(i).wait_send())


def finish_kernel(side, *refs):
    whole, state, new, new_state, write, store = refs[0:3], refs[3:9], refs[9:12], refs[12:18], refs[18], refs[19]
    copies = []
    for k in range(SLICES):
        for layer in range(CORES):
            for q in range(COLORS):
                if q < COLORS // 2:
                    c = whole[k].shape[-1]
                    dst = new[k].at[layer, :, :, q] if k < SLICES - 1 else new[k].at[layer, :, :, :, pl.ds(q * c, c)]
                    copies.append(pltpu.make_async_copy(whole[k].at[layer, q], dst, write.at[k, layer, q, 0]))
                else:
                    for t in range(side):
                        dst = part(new[k], k, layer, q, t, whole[k].shape[-1])
                        copies.append(pltpu.make_async_copy(whole[k].at[layer, q, t], dst, write.at[k, layer, q, t]))
    copies += [pltpu.make_async_copy(src, dst, store.at[i]) for i, (src, dst) in enumerate(zip(state, new_state, strict=True))]
    for copy in copies:
        copy.start()
    for copy in copies:
        copy.wait()


def solution(mesh):
    n = mesh.shape["dp"]
    side = math.isqrt(n // CORES)
    bf16, f32 = jnp.bfloat16, jnp.float32
    shape = jax.ShapeDtypeStruct

    def step(*arrays):
        terms, weights, m, v = (arrays[i : i + 3] for i in (0, 3, 6, 9))
        layers, depth, wide_columns = weights[0].shape
        _, deep, columns = weights[2].shape
        chips = side * side
        high, tall = depth // chips // COLORS, deep // chips
        pieces = [(high, wide_columns)] * 2 + [(tall, columns // COLORS)]
        half = (COLORS, tall // CORES, columns // COLORS)
        count = sum(w.size for w in weights)

        views = [t.reshape(layers, side, side, COLORS, high, wide_columns) for t in terms[:2]]
        views.append(terms[2].reshape(layers, side, side, tall, columns))
        def by_lanes(a):
            layers, rows, columns = a.shape
            a = a.transpose(1, 0, 2).reshape(rows, layers, columns // 128, 128)
            return a.transpose(0, 2, 1, 3).reshape(-1, 128)

        def by_rows(a, like):
            layers, rows, columns = like.shape
            a = a.reshape(rows, columns // 128, layers, 128).transpose(0, 2, 1, 3)
            return a.reshape(rows, layers, columns).transpose(1, 0, 2)

        own = [w.reshape(layers, n, KEPT, high, wide_columns) for w in weights[:2]]
        own.append(weights[2].reshape(layers, chips, tall, columns))
        ms, vs = ([a.reshape(layers, KEPT, high, wide_columns) for a in b[:2]] + [by_lanes(b[2])] for b in (m, v))
        state = [pltpu.VMEM(a.shape, f32) for a in ms]
        gathered = pl.pallas_call(
            functools.partial(step_kernel, side, n, count),
            name="step",
            out_shape=(*(pltpu.VMEM((layers, COLORS, side, side, *p), bf16) for p in pieces), *state, *state),
            in_specs=[ANY] * 12,
            out_specs=(VMEM,) * 9,
            scratch_shapes=[
                *(pltpu.VMEM((COLORS, side - 1, side, *p), bf16) for p in pieces),
                *(pltpu.VMEM((COLORS, side - 1, *p), bf16) for p in pieces),
                *(pltpu.VMEM((COLORS, *p), bf16) for p in pieces[:2]),
                pltpu.VMEM((CORES, *half), bf16),
                *(pltpu.VMEM((KEPT, *p), bf16) for p in pieces[:2]),
                pltpu.VMEM(half, bf16),
                pltpu.VMEM((CORES, *half), bf16),
                pltpu.VMEM(pieces[2], f32),
                pltpu.VMEM((n, 8, 128), f32),
                *(DMA((SLICES, COLORS, side)) for _ in range(3)),
                DMA((SLICES, 2)),
                *(DMA((SLICES, COLORS, side - 1)) for _ in range(4)),
                *(DMA((COLORS, side)) for _ in range(4)),
                *(DMA((n - 1,)) for _ in range(2)),
                *(DMA((SLICES,)) for _ in range(2)),
                DMA((SLICES, CORES, COLORS)),
                *(DMA((SLICES, KEPT)) for _ in range(2)),
                *(DMA((SLICES, COLORS, side - 1)) for _ in range(4)),
                *(DMA((SLICES, COLORS, side)) for _ in range(2)),
                *(DMA((COLORS, side)) for _ in range(4)),
            ],
            compiler_params=pltpu.CompilerParams(collective_id=0, has_side_effects=True, vmem_limit_bytes=22_806_528),
        )(*views, *own, *ms, *vs)
        gathered = [pltpu.with_memory_space_constraint(a, pltpu.VMEM) for a in gathered]
        outs = pl.pallas_call(
            functools.partial(finish_kernel, side),
            name="finish",
            out_shape=tuple(shape(a.shape, a.dtype) for a in (*[shape(t.shape, bf16) for t in views], *ms, *vs)),
            in_specs=[VMEM] * 9,
            out_specs=(ANY,) * 9,
            scratch_shapes=[DMA((SLICES, CORES, COLORS, side)), DMA((2 * SLICES,))],
            compiler_params=pltpu.CompilerParams(vmem_limit_bytes=22_806_528),
        )(*gathered)
        new = [a.reshape(w.shape) for a, w in zip(outs[:3], weights, strict=True)]
        rest = [
            (by_rows(a, like) if i == SLICES - 1 else a.reshape(like.shape))
            for block in (outs[3:6], outs[6:9])
            for i, (a, like) in enumerate(zip(block, m, strict=True))
        ]
        return (*new, *rest)

    all_of, cut = P(None, None, None), P(None, "dp", None)
    return jax.shard_map(
        step,
        mesh=mesh,
        in_specs=(P(("rep", "dp"), None, None, None),) * 3 + (all_of,) * 3 + (cut,) * 6,
        out_specs=(P("rep", None, None),) * 3 + (P("rep", "dp", None),) * 6,
        check_vma=False,
    )
```

```python
import functools
import math

import jax
import jax.numpy as jnp
from jax import lax
from jax.experimental import pallas as pl
from jax.experimental.pallas import tpu as pltpu
from jax.sharding import PartitionSpec as P

MESH = pl.DeviceIdType.MESH
CORES = 2
COLORS = 4
SLICES = 3
KEPT = COLORS // CORES
ANY = pl.BlockSpec(memory_space=pl.ANY)
VMEM = pl.BlockSpec(memory_space=pltpu.VMEM)
DMA = pltpu.SemaphoreType.DMA


def each(n, body):
    lax.fori_loop(0, n, lambda i, _: body(i), None)


class Place:
    def __init__(self, side):
        self.side = side
        self.me = lax.axis_index("dp")
        self.core = lax.rem(self.me, CORES)
        self.chip = self.me // CORES
        self.x, self.y = self.chip // side, lax.rem(self.chip, side)
        self.partner = self.me + 1 - 2 * self.core

    def at(self, x, y):
        return (x * self.side + y) * CORES + self.core

    def moved(self, p, by):
        return lax.rem(p + by + 2 * self.side, self.side)

    def way(self, q):
        on_x = q < COLORS // 2
        return jnp.where(on_x, self.x, self.y), jnp.where(on_x, self.y, self.x), 1 - 2 * lax.rem(q, 2)

    def next(self, q, first):
        up = 1 - 2 * lax.rem(q, 2)
        on_x = (q < COLORS // 2) == first
        return self.at(jnp.where(on_x, self.moved(self.x, up), self.x), jnp.where(on_x, self.y, self.moved(self.y, up)))


def remote(src, dst, send, recv, device):
    return pltpu.make_async_remote_copy(
        src_ref=src, dst_ref=dst, send_sem=send, recv_sem=recv, device_id={"dp": device}, device_id_type=MESH
    )


def meet(at):
    barrier = pltpu.get_barrier_semaphore()
    near = [at.partner] + [at.next(q, True) for q in range(COLORS)]
    for device in near:
        pl.semaphore_signal(barrier, inc=1, device_id={"dp": device}, device_id_type=MESH)
    return lambda: pl.semaphore_wait(barrier, len(near))


def part(ref, k, layer, q, t, columns):
    if k < SLICES - 1:
        return ref.at[layer, t, :, q] if q < COLORS // 2 else ref.at[layer, :, t, q]
    c = pl.ds(q * columns, columns)
    return ref.at[layer, t, :, :, c] if q < COLORS // 2 else ref.at[layer, :, t, :, c]


def wide(x):
    return x.astype(jnp.float32)


def squares(g):
    total = jnp.zeros((8, 128), jnp.float32)
    for r in range(0, g.shape[0], 8):
        for c in range(0, g.shape[1], 128):
            block = g[r : r + 8, c : c + 128]
            total += block * block
    return total


def factor_of(total, count):
    return jnp.minimum(1.0, 0.5 * lax.rsqrt(jnp.sum(total) / count + 1e-30))


def moments(m, v, g):
    return 0.9 * m + 0.1 * g, 0.95 * v + 0.05 * g * g


def new_weight(w, m, v, g):
    m, v = moments(m, v, g)
    return (w - 0.02 * (m * lax.rsqrt(v + 1e-8) + 0.1 * w)).astype(jnp.bfloat16)


def lanes_of(layers, rows, q, columns, layer):
    per_row = COLORS * columns // 128 * layers
    return [pl.ds((q * columns // 128 + i) * layers + layer, rows, stride=per_row) for i in range(columns // 128)]


def step_kernel(side, n, count, *refs):
    terms, weights, m, v = refs[0:3], refs[3:6], refs[6:9], refs[9:12]
    out, mb, vb = refs[12:15], refs[15:18], refs[18:21]
    r1, r2, fin, lent_sums = refs[21:24], refs[24:27], refs[27:30], refs[30:33]
    half_w, tmp, norms = refs[33:36]
    load, push_s, push_r, state_in = refs[36:40]
    s1, v1, s2, v2 = refs[40:44]
    piece_s, piece_r, s1_piece, v1_piece = refs[44:48]
    norm_s, norm_r, sum_s, sum_r = refs[48:52]
    rows_in, swap_s, swap_r = refs[52:55]
    t1, u1, t2, u2 = refs[55:59]
    give_s, give_r, t2_piece, u2_piece, give_piece_s, give_piece_r = refs[59:65]
    at = Place(side)
    me, core, partner = at.me, at.core, at.partner
    other = 1 - core
    last = side - 1
    down = SLICES - 1
    rows, columns = half_w.shape[-2:]

    def group(q, s):
        p1, _, up = at.way(q)
        return at.moved(p1, -up * (1 + s))

    def loads(k, s):
        for q in range(COLORS):
            t = group(q, s)
            pltpu.make_async_copy(part(terms[k], k, core, q, t, columns), out[k].at[core, q, t], load.at[k, q, s]).start()

    def pushed(k, q, s, src=None):
        dst = out[k].at[core, q, group(q, s)]
        return remote(dst if src is None else src, dst, push_s.at[k, q, s], push_r.at[k, q, s], partner)

    def pushes(k, s):
        for q in range(COLORS):
            pushed(k, q, s, part(terms[k], k, other, q, group(q, s), columns)).start()

    def loaded(k, q, s):
        ref = out[k].at[core, q, group(q, s)]
        pltpu.make_async_copy(ref, ref, load.at[k, q, s]).wait()

    def ready(k, q, s):
        loaded(k, q, s)
        pushed(k, q, s).wait_recv()

    def pushed_piece(q, j, src=None):
        dst = out[0].at[core, q, group(q, 0), j]
        return remote(dst if src is None else src, dst, piece_s.at[q, j], piece_r.at[q, j], partner)

    def sum1_piece(q, j):
        src = out[0].at[core, q, group(q, 0), j]
        return remote(src, r1[0].at[q, 0, j], s1_piece.at[q, j], v1_piece.at[q, j], at.next(q, True))

    def sum1(k, q, s):
        src = r1[k].at[q, s - 1] if s else out[k].at[core, q, group(q, s)]
        return remote(src, r1[k].at[q, s], s1.at[k, q, s], v1.at[k, q, s], at.next(q, True))

    def sum2(k, q, s):
        _, p2, up = at.way(q)
        src = r2[k].at[q, s - 1] if s else r1[k].at[q, last - 1, at.moved(p2, -up)]
        return remote(src, r2[k].at[q, s], s2.at[k, q, s], v2.at[k, q, s], at.next(q, False))

    greet = meet(at)
    for k in range(SLICES):
        loads(k, 0)
    greet()
    for j in range(side):
        for q in range(COLORS):
            pushed_piece(q, j, part(terms[0], 0, other, q, group(q, 0), columns).at[j]).start()
    for k in range(1, SLICES):
        pushes(k, 0)

    def both(k, q, t, j):
        return wide(out[k][0, q, t, j]) + wide(out[k][1, q, t, j])

    for j in range(side):

        def start(q):
            t = group(q, 0)
            if j == 0:
                loaded(0, q, 0)
            pushed_piece(q, j).wait_recv()
            out[0][core, q, t, j] = both(0, q, t, j).astype(jnp.bfloat16)
            sum1_piece(q, j).start()

        each(COLORS, start)
    loads(0, 1)
    pushes(0, 1)
    for s in range(last):
        for k in range(SLICES):
            if s == 0 and k == 0:
                continue

            def first(q):
                t = group(q, s)
                if s == 1 and k == 0:
                    each(side, lambda j: sum1_piece(q, j).wait_recv())
                elif s:
                    sum1(k, q, s - 1).wait_recv()
                ready(k, q, s)

                def add(j):
                    if s:
                        r1[k][q, s - 1, j] = (wide(r1[k][q, s - 1, j]) + both(k, q, t, j)).astype(jnp.bfloat16)
                    else:
                        out[k][core, q, t, j] = both(k, q, t, j).astype(jnp.bfloat16)

                each(side, add)
                sum1(k, q, s).start()

            each(COLORS, first)
            loads(k, s + 1)
            pushes(k, s + 1)
        if s == 0:
            moments_in = [
                pltpu.make_async_copy(src[k], dst[k], state_in.at[k, i])
                for k in range(SLICES)
                for i, (src, dst) in enumerate(((m, mb), (v, vb)))
            ]
            for copy in moments_in:
                copy.start()

    def here(k, q, u):
        p1, _, _ = at.way(q)
        return both(k, q, p1, u) + wide(r1[k][q, last - 1, u])

    for s in range(last):
        for k in range(SLICES):

            def second(q):
                _, p2, up = at.way(q)
                u = at.moved(p2, -up * (1 + s))
                if s:
                    sum2(k, q, s - 1).wait_recv()
                    r2[k][q, s - 1] = (wide(r2[k][q, s - 1]) + here(k, q, u)).astype(jnp.bfloat16)
                else:
                    sum1(k, q, last - 1).wait_recv()
                    ready(k, q, last)
                    r1[k][q, last - 1, u] = here(k, q, u).astype(jnp.bfloat16)
                sum2(k, q, s).start()

            each(COLORS, second)

    def share(k, of):
        return fin[k].at[pl.ds(of * KEPT, KEPT)] if k < down else fin[k].at[of]

    def swap_sums(k):
        return remote(share(k, other), lent_sums[k], sum_s.at[k], sum_r.at[k], partner)

    def norm(i):
        return remote(norms.at[me], norms.at[me], norm_s.at[i], norm_r.at[i], lax.rem(me + 1 + i, n))

    norms[me] = jnp.zeros((8, 128), jnp.float32)
    for k in range(SLICES):

        def end(q):
            _, p2, _ = at.way(q)
            sum2(k, q, last - 1).wait_recv()
            g = (wide(r2[k][q, last - 1]) + here(k, q, p2)).astype(jnp.bfloat16)
            norms[me] += squares(wide(g))
            if k < down:
                fin[k][q] = g
            else:
                r2[k][q, last - 1] = g

            if k:
                sum1(k, q, 0).wait_send()
            else:
                each(side, lambda j: sum1_piece(q, j).wait_send())

        each(COLORS, end)
        if k < down:
            swap_sums(k).start()
    each(n - 1, lambda i: norm(i).start())

    def halve(q):
        tmp[...] = wide(r2[down][q, last - 1])
        for h in range(CORES):
            fin[down][h, q] = tmp[h * rows : (h + 1) * rows].astype(jnp.bfloat16)

    each(COLORS, halve)
    swap_sums(down).start()
    for k in range(SLICES):

        def drain(q):
            for s in range(side):
                if k or s:
                    pushed(k, q, s).wait_send()
            for s in range(last):
                if s:
                    sum1(k, q, s).wait_send()
                sum2(k, q, s).wait_send()
            if k == 0:
                each(side, lambda j: pushed_piece(q, j).wait_send())

        each(COLORS, drain)

    def old(k, layer, i):
        return r1[k].at[0, 0, layer * KEPT + i] if k < down else r1[k].at[layer, 0, i]

    def rows_of(k):
        for layer in range(CORES):
            for i in range(KEPT if k < down else COLORS):
                if k < down:
                    src = weights[k].at[layer, me, i]
                else:
                    src = weights[k].at[layer, at.chip, :, pl.ds(i * columns, columns)]
                yield pltpu.make_async_copy(src, old(k, layer, i), rows_in.at[k, layer, i])

    for k in range(SLICES):
        for copy in rows_of(k):
            copy.start()
    for copy in moments_in:
        copy.wait()
    for k in range(SLICES):
        swap_sums(k).wait_recv()
        for copy in rows_of(k):
            copy.wait()
    each(n - 1, lambda i: norm(i).wait_recv())
    factor = factor_of(jnp.sum(norms[...], axis=0), count)

    def swap(k, i, q, layer):
        p1, p2, _ = at.way(q)
        return remote(r2[k].at[i, 0], out[k].at[layer, q, p1, p2], swap_s.at[k, i], swap_r.at[k, i], partner)

    def hop1(k, q, s):
        p1, p2, up = at.way(q)
        ref = out[k].at[core, q, p1, at.moved(p2, -up * s)]
        return remote(ref, ref, t1.at[k, q, s], u1.at[k, q, s], at.next(q, False))

    def hop2(k, q, s):
        p1, _, up = at.way(q)
        ref = out[k].at[core, q, at.moved(p1, -up * s)]
        return remote(ref, ref, t2.at[k, q, s], u2.at[k, q, s], at.next(q, True))

    def give(k, q, s, layer):
        p1, _, up = at.way(q)
        ref = out[k].at[layer, q, at.moved(p1, -up * s)]
        return remote(ref, ref, give_s.at[k, q, s], give_r.at[k, q, s], partner)

    def hop2_piece(q, j):
        p1, _, up = at.way(q)
        ref = out[down].at[core, q, at.moved(p1, -up * (last - 1)), j]
        return remote(ref, ref, t2_piece.at[q, j], u2_piece.at[q, j], at.next(q, True))

    def give_piece(q, j, layer):
        p1, _, up = at.way(q)
        ref = out[down].at[layer, q, at.moved(p1, -up * last), j]
        return remote(ref, ref, give_piece_s.at[q, j], give_piece_r.at[q, j], partner)

    def gradient(k, mine, i):
        if k < down:
            return wide(fin[k][core * KEPT + i] if mine else lent_sums[k][i]) * factor
        return wide(fin[k][core, i] if mine else lent_sums[k][i]) * factor

    def step(k):
        for layer, mine in ((core, True), (other, False)):
            for i in range(KEPT):
                q = core * KEPT + i
                w = new_weight(wide(old(k, layer, i)[...]), mb[k][layer, i], vb[k][layer, i], gradient(k, mine, i))
                if mine:
                    p1, p2, _ = at.way(q)
                    out[k][layer, q, p1, p2] = w
                    hop1(k, q, 0).start()
                else:
                    r2[k][i, 0] = w
                    swap(k, i, q, other).start()

    def swapped(k):
        for i in range(KEPT):
            q = other * KEPT + i
            swap(k, i, q, core).wait_recv()
            hop1(k, q, 0).start()

    half_swap = remote(fin[down].at[other], half_w.at[1], swap_s.at[down, 0], swap_r.at[down, 0], partner)

    def for_layer(mine, body):
        for layer in range(CORES):
            pl.when((layer == core) == mine)(functools.partial(body, layer))

    def step_down(mine):
        def body(layer):
            for q in range(COLORS):
                tmp[...] = wide(old(down, layer, q)[...])
                w = jnp.where(core == 0, tmp[0:rows], tmp[rows : 2 * rows])
                where = lanes_of(CORES, rows, q, columns, layer)
                one = jnp.concatenate([mb[down][i, :] for i in where], axis=1)
                two = jnp.concatenate([vb[down][i, :] for i in where], axis=1)
                w = new_weight(w, one, two, gradient(down, mine, q))
                if mine:
                    half_w[0, q] = w
                else:
                    fin[down][other, q] = w

        for_layer(mine, body)

    def keep_moments(k):
        for mine in (True, False):
            if k < down:
                layer = core if mine else other
                for i in range(KEPT):
                    one, two = moments(mb[k][layer, i], vb[k][layer, i], gradient(k, mine, i))
                    mb[k][layer, i] = one
                    vb[k][layer, i] = two
                continue

            def body(layer, mine=mine):
                for q in range(COLORS):
                    g = gradient(down, mine, q)
                    for i, where in enumerate(lanes_of(CORES, rows, q, columns, layer)):
                        one, two = moments(mb[k][where, :], vb[k][where, :], g[:, i * 128 : (i + 1) * 128])
                        mb[k][where, :] = one
                        vb[k][where, :] = two

            for_layer(mine, body)

    step(0)
    step(1)
    swapped(0)
    swap_sums(down).wait_send()
    step_down(False)
    half_swap.start()
    swapped(1)
    step_down(True)
    half_swap.wait_recv()
    for q in range(COLORS):
        p1, p2, _ = at.way(q)
        tmp[0:rows] = wide(half_w[core, q])
        tmp[rows : 2 * rows] = wide(half_w[other, q])
        out[down][core, q, p1, p2] = tmp[...].astype(jnp.bfloat16)
        hop1(down, q, 0).start()

    for s in range(1, last):
        for k in range(SLICES):

            def spread(q):
                hop1(k, q, s - 1).wait_recv()
                hop1(k, q, s).start()

            each(COLORS, spread)
    for s in range(side):
        for k in range(SLICES):

            def onward(q):
                if s:
                    hop2(k, q, s - 1).wait_recv()
                else:
                    hop1(k, q, last - 1).wait_recv()
                if k == down and s == last - 1:
                    each(side, lambda j: hop2_piece(q, j).start())
                elif s < last:
                    hop2(k, q, s).start()
                give(k, q, s, core).start()

            def onward_piece(i):
                j, q = i // COLORS, lax.rem(i, COLORS)
                hop2_piece(q, j).wait_recv()
                give_piece(q, j, core).start()

            if k == down and s == last:
                each(side * COLORS, onward_piece)
            else:
                each(COLORS, onward)
            if s == 0:
                keep_moments(k)

    for k in range(SLICES):

        def settle(q):
            cut = 1 if k == down else 0
            for s in range(side - cut):
                give(k, q, s, other).wait_recv()
                give(k, q, s, core).wait_send()
            for s in range(last):
                hop1(k, q, s).wait_send()
                if s < last - cut:
                    hop2(k, q, s).wait_send()
            if cut:

                def pieces(j):
                    give_piece(q, j, other).wait_recv()
                    give_piece(q, j, core).wait_send()
                    hop2_piece(q, j).wait_send()

                each(side, pieces)

        each(COLORS, settle)
        if k < down:
            swap_sums(k).wait_send()
            for i in range(KEPT):
                swap(k, i, core * KEPT + i, other).wait_send()
    half_swap.wait_send()
    each(n - 1, lambda i: norm(i).wait_send())


def finish_kernel(side, *refs):
    whole, state, new, new_state, write, store = refs[0:3], refs[3:9], refs[9:12], refs[12:18], refs[18], refs[19]
    for k in range(SLICES):
        for layer in range(CORES):
            for q in range(COLORS):
                if q < COLORS // 2:
                    c = whole[k].shape[-1]
                    dst = new[k].at[layer, :, :, q] if k < SLICES - 1 else new[k].at[layer, :, :, :, pl.ds(q * c, c)]
                    pltpu.make_async_copy(whole[k].at[layer, q], dst, write.at[k]).start()
                else:
                    for t in range(side):
                        dst = part(new[k], k, layer, q, t, whole[k].shape[-1])
                        pltpu.make_async_copy(whole[k].at[layer, q, t], dst, write.at[k]).start()
        for i in (k, k + SLICES):
            pltpu.make_async_copy(state[i], new_state[i], store.at[i]).start()
    for k in range(SLICES):
        pltpu.make_async_copy(whole[k], whole[k], write.at[k]).wait()
    for i in range(2 * SLICES):
        pltpu.make_async_copy(state[i], new_state[i], store.at[i]).wait()


def solution(mesh):
    n = mesh.shape["dp"]
    side = math.isqrt(n // CORES)
    bf16, f32 = jnp.bfloat16, jnp.float32
    shape = jax.ShapeDtypeStruct

    def step(*arrays):
        terms, weights, m, v = (arrays[i : i + 3] for i in (0, 3, 6, 9))
        layers, depth, wide_columns = weights[0].shape
        _, deep, columns = weights[2].shape
        chips = side * side
        high, tall = depth // chips // COLORS, deep // chips
        pieces = [(high, wide_columns)] * 2 + [(tall, columns // COLORS)]
        half = (COLORS, tall // CORES, columns // COLORS)
        count = sum(w.size for w in weights)

        views = [t.reshape(layers, side, side, COLORS, high, wide_columns) for t in terms[:2]]
        views.append(terms[2].reshape(layers, side, side, tall, columns))
        def by_lanes(a):
            layers, rows, columns = a.shape
            a = a.transpose(1, 0, 2).reshape(rows, layers, columns // 128, 128)
            return a.transpose(0, 2, 1, 3).reshape(-1, 128)

        def by_rows(a, like):
            layers, rows, columns = like.shape
            a = a.reshape(rows, columns // 128, layers, 128).transpose(0, 2, 1, 3)
            return a.reshape(rows, layers, columns).transpose(1, 0, 2)

        own = [w.reshape(layers, n, KEPT, high, wide_columns) for w in weights[:2]]
        own.append(weights[2].reshape(layers, chips, tall, columns))
        ms, vs = ([a.reshape(layers, KEPT, high, wide_columns) for a in b[:2]] + [by_lanes(b[2])] for b in (m, v))
        state = [pltpu.VMEM(a.shape, f32) for a in ms]
        gathered = pl.pallas_call(
            functools.partial(step_kernel, side, n, count),
            name="step",
            out_shape=(*(pltpu.VMEM((layers, COLORS, side, side, *p), bf16) for p in pieces), *state, *state),
            in_specs=[ANY] * 12,
            out_specs=(VMEM,) * 9,
            scratch_shapes=[
                *(pltpu.VMEM((COLORS, side - 1, side, *p), bf16) for p in pieces),
                *(pltpu.VMEM((COLORS, side - 1, *p), bf16) for p in pieces),
                *(pltpu.VMEM((COLORS, *p), bf16) for p in pieces[:2]),
                pltpu.VMEM((CORES, *half), bf16),
                *(pltpu.VMEM((KEPT, *p), bf16) for p in pieces[:2]),
                pltpu.VMEM(half, bf16),
                pltpu.VMEM((CORES, *half), bf16),
                pltpu.VMEM(pieces[2], f32),
                pltpu.VMEM((n, 8, 128), f32),
                *(DMA((SLICES, COLORS, side)) for _ in range(3)),
                DMA((SLICES, 2)),
                *(DMA((SLICES, COLORS, side - 1)) for _ in range(4)),
                *(DMA((COLORS, side)) for _ in range(4)),
                *(DMA((n - 1,)) for _ in range(2)),
                *(DMA((SLICES,)) for _ in range(2)),
                DMA((SLICES, CORES, COLORS)),
                *(DMA((SLICES, KEPT)) for _ in range(2)),
                *(DMA((SLICES, COLORS, side - 1)) for _ in range(4)),
                *(DMA((SLICES, COLORS, side)) for _ in range(2)),
                *(DMA((COLORS, side)) for _ in range(4)),
            ],
            compiler_params=pltpu.CompilerParams(collective_id=0, has_side_effects=True, vmem_limit_bytes=22_806_528),
        )(*views, *own, *ms, *vs)
        gathered = [pltpu.with_memory_space_constraint(a, pltpu.VMEM) for a in gathered]
        outs = pl.pallas_call(
            functools.partial(finish_kernel, side),
            name="finish",
            out_shape=tuple(shape(a.shape, a.dtype) for a in (*[shape(t.shape, bf16) for t in views], *ms, *vs)),
            in_specs=[VMEM] * 9,
            out_specs=(ANY,) * 9,
            scratch_shapes=[DMA((SLICES,)), DMA((2 * SLICES,))],
            compiler_params=pltpu.CompilerParams(vmem_limit_bytes=22_806_528),
        )(*gathered)
        new = [a.reshape(w.shape) for a, w in zip(outs[:3], weights, strict=True)]
        rest = [
            (by_rows(a, like) if i == SLICES - 1 else a.reshape(like.shape))
            for block in (outs[3:6], outs[6:9])
            for i, (a, like) in enumerate(zip(block, m, strict=True))
        ]
        return (*new, *rest)

    all_of, cut = P(None, None, None), P(None, "dp", None)
    return jax.shard_map(
        step,
        mesh=mesh,
        in_specs=(P(("rep", "dp"), None, None, None),) * 3 + (all_of,) * 3 + (cut,) * 6,
        out_specs=(P("rep", None, None),) * 3 + (P("rep", "dp", None),) * 6,
        check_vma=False,
    )
```
